16 devices in a mesh: dp: 2 (over z), tp: 8 (over y, x, core).
Axes of the slice: x: 2, y: 2, z: 2, core: 2. Of those that a mesh axis runs over, the one named last changes fastest.
Arguments:
- x_tokens: bfloat16 [32, 512, 3072], P('dp', 'tp'), parts along dimension 0
- e_time: float32 [32, 3, 3072], P('dp'), parts along dimension 0
- m_block: float32 [3, 3072], replicated
- w_q: bfloat16 [3072, 3072], P(None, 'tp')
- b_q: float32 [3072], P('tp')
- w_k: bfloat16 [3072, 3072], P(None, 'tp')
- b_k: float32 [3072], P('tp')
- w_v: bfloat16 [3072, 3072], P(None, 'tp')
- b_v: float32 [3072], P('tp')
- w_o: bfloat16 [3072, 3072], P('tp')
- b_o: float32 [3072], replicated
- g_q: float32 [3072], P('tp')
- g_k: float32 [3072], P('tp')
- positions: int32 [1024, 3], P('dp'), parts along dimension 0
- d_out: bfloat16 [32, 512, 3072], P('dp', 'tp'), parts along dimension 0
Outputs:
- output 1: bfloat16 [32, 512, 3072], P('dp', 'tp'), parts along dimension 0
- output 2: bfloat16 [32, 512, 3072], P('dp', 'tp'), parts along dimension 0
- output 3: float32 [32, 3, 3072], P('dp'), parts along dimension 0
- output 4: float32 [6, 3072], P('dp'), parts along dimension 0
- output 5: bfloat16 [6144, 3072], P('dp', 'tp'), parts along dimension 0
- output 6: bfloat16 [6144, 3072], P('dp', 'tp'), parts along dimension 0
- output 7: bfloat16 [6144, 3072], P('dp', 'tp'), parts along dimension 0
- output 8: bfloat16 [6144, 3072], P(('dp', 'tp')), parts along dimension 0
- output 9: float32 [6144], P(('dp', 'tp')), parts along dimension 0
- output 10: float32 [6144], P(('dp', 'tp')), parts along dimension 0
There are 2 independent parts. The reference program is written for one: setup_inputs(seed, part) draws one part's arguments, and reference() takes and returns one part's arrays. A program takes and returns all parts, laid end to end along the dimension named above; an argument that names none is the same for every part.
All inputs are finite; a program needn't handle non-finite values.
Results may differ from the reference program's by a relative error of at most 0.0197529.
Values are sent between devices in bfloat16 or wider.
A program may use at most 1 GiB of HBM per device.

```python
import jax
import jax.numpy as jnp
from jax import lax

NUM_BATCH = 16
SEQ_LEN = 512
NUM_HEADS = 24
HEAD_DIM = 128
MODEL_DIM = 3072
NUM_FRAMES = 21
NUM_ROWS = 45
NUM_COLS = 80

EPS_NORM = 1e-6
ROPE_BASE = 10000.0


def draw_positions(pos_key):
    coord_keys = jax.random.split(pos_key, 3)
    frame_ids = jax.random.randint(coord_keys[0], (SEQ_LEN,), 0, NUM_FRAMES)
    row_ids = jax.random.randint(coord_keys[1], (SEQ_LEN,), 0, NUM_ROWS)
    col_ids = jax.random.randint(coord_keys[2], (SEQ_LEN,), 0, NUM_COLS)
    grid_pos = jnp.stack([frame_ids, row_ids, col_ids], axis=1).astype(jnp.int32)
    corner_hi = jnp.array([NUM_FRAMES - 1, NUM_ROWS - 1, NUM_COLS - 1], dtype=jnp.int32)
    return grid_pos.at[0].set(corner_hi).at[1].set(jnp.zeros((3,), jnp.int32))


def setup_inputs(seed: int = 0, part: int = 0) -> dict:
    root_key = jax.random.key(seed)
    shared_keys = jax.random.split(root_key, 12)
    part_keys = jax.random.split(jax.random.fold_in(root_key, part), 4)
    fan_scale = MODEL_DIM ** -0.5
    head_ramp = 2.0 ** (2.0 * jnp.arange(NUM_HEADS, dtype=jnp.float32) / max(NUM_HEADS - 1, 1) - 1.0)
    col_scale = jnp.repeat(head_ramp, HEAD_DIM)
    sq_shape = (MODEL_DIM, MODEL_DIM)
    vec_shape = (MODEL_DIM,)
    tok_shape = (NUM_BATCH, SEQ_LEN, MODEL_DIM)
    return {
        'x_tokens': (0.5 * jax.random.normal(part_keys[0], tok_shape, jnp.float32)).astype(jnp.bfloat16),
        'e_time': 0.5 * jax.random.normal(part_keys[1], (NUM_BATCH, 3, MODEL_DIM), jnp.float32),
        'm_block': 0.5 * jax.random.normal(shared_keys[0], (3, MODEL_DIM), jnp.float32),
        'w_q': (jax.random.normal(shared_keys[1], sq_shape, jnp.float32) * fan_scale * col_scale).astype(jnp.bfloat16),
        'b_q': 0.5 * jax.random.normal(shared_keys[2], vec_shape, jnp.float32),
        'w_k': (jax.random.normal(shared_keys[3], sq_shape, jnp.float32) * fan_scale * col_scale).astype(jnp.bfloat16),
        'b_k': 0.5 * jax.random.normal(shared_keys[4], vec_shape, jnp.float32),
        'w_v': (jax.random.normal(shared_keys[5], sq_shape, jnp.float32) * (1.5 * fan_scale)).astype(jnp.bfloat16),
        'b_v': 0.5 * jax.random.normal(shared_keys[6], vec_shape, jnp.float32),
        'w_o': (jax.random.normal(shared_keys[7], sq_shape, jnp.float32) * fan_scale).astype(jnp.bfloat16),
        'b_o': 0.5 * jax.random.normal(shared_keys[8], vec_shape, jnp.float32),
        'g_q': jax.random.uniform(shared_keys[9], vec_shape, jnp.float32, 0.5, 1.5),
        'g_k': jax.random.uniform(shared_keys[10], vec_shape, jnp.float32, 0.5, 1.5),
        'positions': draw_positions(part_keys[3]),
        'd_out': jax.random.normal(part_keys[2], tok_shape, jnp.float32).astype(jnp.bfloat16),
    }


def rope_angles(positions):
    half_dim = HEAD_DIM // 2
    side_len = HEAD_DIM // 6
    first_len = half_dim - 2 * side_len
    pair_idx = jnp.arange(half_dim)
    section = (pair_idx >= first_len).astype(jnp.int32) + (pair_idx >= first_len + side_len).astype(jnp.int32)
    offset = jnp.where(section == 0, 0, jnp.where(section == 1, first_len, first_len + side_len))
    sec_width = jnp.where(section == 0, first_len, side_len)
    freq_vals = ROPE_BASE ** (-(pair_idx - offset).astype(jnp.float32) / sec_width.astype(jnp.float32))
    select = jnp.where(section[None, :] == jnp.arange(3)[:, None], freq_vals[None, :], 0.0)
    angles = jnp.sum(positions.astype(jnp.float32)[:, :, None] * select[None, :, :], axis=1)
    return jnp.cos(angles), jnp.sin(angles)


def rope_rotate(values, cos_part, sin_part):
    val_pairs = values.reshape(values.shape[:-1] + (values.shape[-1] // 2, 2))
    even_part = val_pairs[..., 0]
    odd_part = val_pairs[..., 1]
    rotated = jnp.stack([even_part * cos_part - odd_part * sin_part, even_part * sin_part + odd_part * cos_part], axis=-1)
    return rotated.reshape(values.shape)


def full_rms(values, gain):
    return values * lax.rsqrt(jnp.mean(values * values, axis=-1, keepdims=True) + EPS_NORM) * gain


def head_attention(operands):
    q_head, k_head, v_head = operands
    scores = jnp.einsum('bqd,bkd->bqk', q_head.astype(jnp.float32), k_head.astype(jnp.float32)) * HEAD_DIM ** -0.5
    attn_probs = jax.nn.softmax(scores, axis=-1).astype(jnp.bfloat16)
    return jnp.einsum('bqk,bkd->bqd', attn_probs.astype(jnp.float32), v_head.astype(jnp.float32)).astype(jnp.bfloat16)


def attention_block(x_tokens, e_time, m_block, w_q, b_q, w_k, b_k, w_v, b_v, w_o, b_o, g_q, g_k, cos_bcast, sin_bcast):
    head_shape = (NUM_BATCH, SEQ_LEN, NUM_HEADS, HEAD_DIM)
    mod_rows = m_block[None] + e_time
    shift_row = mod_rows[:, 0][:, None]
    scale_one = 1.0 + mod_rows[:, 1][:, None]
    gate_row = mod_rows[:, 2][:, None]
    x_float = x_tokens.astype(jnp.float32)
    centered = x_float - jnp.mean(x_float, axis=-1, keepdims=True)
    x_norm = centered * lax.rsqrt(jnp.mean(centered * centered, axis=-1, keepdims=True) + EPS_NORM)
    y_act = (x_norm * scale_one + shift_row).astype(jnp.bfloat16).reshape(NUM_BATCH * SEQ_LEN, MODEL_DIM)
    q_raw = jnp.dot(y_act, w_q, preferred_element_type=jnp.float32) + b_q
    k_raw = jnp.dot(y_act, w_k, preferred_element_type=jnp.float32) + b_k
    v_heads = (jnp.dot(y_act, w_v, preferred_element_type=jnp.float32) + b_v).astype(jnp.bfloat16).reshape(head_shape)
    q_rot = rope_rotate(full_rms(q_raw, g_q).reshape(head_shape), cos_bcast, sin_bcast).astype(jnp.bfloat16)
    k_rot = rope_rotate(full_rms(k_raw, g_k).reshape(head_shape), cos_bcast, sin_bcast).astype(jnp.bfloat16)
    o_heads = lax.map(jax.checkpoint(head_attention), (jnp.moveaxis(q_rot, 2, 0), jnp.moveaxis(k_rot, 2, 0), jnp.moveaxis(v_heads, 2, 0)))
    o_flat = jnp.moveaxis(o_heads, 0, 2).reshape(NUM_BATCH * SEQ_LEN, MODEL_DIM)
    proj_out = (jnp.dot(o_flat, w_o, preferred_element_type=jnp.float32) + b_o).reshape(NUM_BATCH, SEQ_LEN, MODEL_DIM)
    return (x_float + gate_row * proj_out).astype(jnp.bfloat16)


def reference(x_tokens, e_time, m_block, w_q, b_q, w_k, b_k, w_v, b_v, w_o, b_o, g_q, g_k, positions, d_out):
    cos_tab, sin_tab = rope_angles(positions)
    cos_bcast = cos_tab[None, :, None, :]
    sin_bcast = sin_tab[None, :, None, :]

    def block_fn(x_in, e_in, m_in, wq_in, wk_in, wv_in, wo_in, gq_in, gk_in):
        return attention_block(x_in, e_in, m_in, wq_in, b_q, wk_in, b_k, wv_in, b_v, wo_in, b_o, gq_in, gk_in, cos_bcast, sin_bcast)

    x_out, pull_back = jax.vjp(block_fn, x_tokens, e_time, m_block, w_q, w_k, w_v, w_o, g_q, g_k)
    d_x, d_e, d_m, d_wq, d_wk, d_wv, d_wo, d_gq, d_gk = pull_back(d_out)
    return (x_out, d_x, d_e, d_m, d_wq, d_wk, d_wv, d_wo, d_gq, d_gk)
```

```python
import functools

import jax
import jax.numpy as jnp
from jax import lax
from jax.experimental import pallas as pl
from jax.experimental.pallas import tpu as pltpu
from jax.sharding import PartitionSpec as P

HEAD_DIM = 128
EPS_NORM = 1e-6
ROPE_BASE = 10000.0
ROW_CONTRACT = (((0,), (0,)), ((), ()))
COL_CONTRACT = (((1,), (1,)), ((), ()))
MESH = pl.DeviceIdType.MESH
F32 = jnp.float32
BF16 = jnp.bfloat16
LOOKAHEAD = 2


def rope_angles(positions):
    half_dim = HEAD_DIM // 2
    side_len = HEAD_DIM // 6
    first_len = half_dim - 2 * side_len
    pair_idx = jnp.arange(half_dim)
    section = (pair_idx >= first_len).astype(jnp.int32) + (pair_idx >= first_len + side_len).astype(jnp.int32)
    offset = jnp.where(section == 0, 0, jnp.where(section == 1, first_len, first_len + side_len))
    sec_width = jnp.where(section == 0, first_len, side_len)
    freq_vals = ROPE_BASE ** (-(pair_idx - offset).astype(jnp.float32) / sec_width.astype(jnp.float32))
    select = jnp.where(section[None, :] == jnp.arange(3)[:, None], freq_vals[None, :], 0.0)
    angles = jnp.sum(positions.astype(jnp.float32)[:, :, None] * select[None, :, :], axis=1)
    return jnp.cos(angles), jnp.sin(angles)


def rope_rotate(values, cos_part, sin_part):
    val_pairs = values.reshape(values.shape[:-1] + (values.shape[-1] // 2, 2))
    even_part = val_pairs[..., 0]
    odd_part = val_pairs[..., 1]
    rotated = jnp.stack([even_part * cos_part - odd_part * sin_part, even_part * sin_part + odd_part * cos_part], axis=-1)
    return rotated.reshape(values.shape)


def attend(q_rot, k_rot, v_heads):
    scores = jnp.einsum('bqhd,bkhd->bhqk', q_rot, k_rot, preferred_element_type=jnp.float32) * HEAD_DIM ** -0.5
    attn_probs = jax.nn.softmax(scores, axis=-1).astype(jnp.bfloat16)
    return jnp.einsum('bhqk,bkhd->bqhd', attn_probs, v_heads, preferred_element_type=jnp.float32).astype(jnp.bfloat16)


class Peers:
    def __init__(self):
        me = lax.axis_index('tp')
        self.me = me
        core, col, row = lax.rem(me, 2), lax.rem(me // 2, 2), me // 4
        self.core, self.col, self.row = core, col, row

        def flip(bits):
            out = me
            if bits & 1:
                out = out + 1 - 2 * core
            if bits & 2:
                out = out + 2 - 4 * col
            if bits & 4:
                out = out + 4 - 8 * row
            return out

        self.at = [flip(bits) for bits in range(8)]


def entry_barrier(peers, which):
    barrier = pltpu.get_barrier_semaphore()
    for bits in which:
        pl.semaphore_signal(barrier, inc=1, device_id={'tp': peers.at[bits]}, device_id_type=MESH)
    pl.semaphore_wait(barrier, len(which))


def wait_bytes(ref, sem):
    pltpu.make_async_copy(ref, ref, sem).wait()


class RowGather:
    def __init__(self, peers, src, full, sems):
        self.peers, self.src, self.full = peers, src, full
        self.send_sem, self.rx, self.ry, self.rd0, self.rd1, self.rp = sems
        self.seg = src.shape[1]

    def piece(self, b, t, lo=0, n=None):
        n = self.seg if n is None else n
        return self.full.at[b, pl.ds(pl.multiple_of(t * self.seg + lo, 32), n), :]

    def send(self, src, dst, b, sem, bits):
        pltpu.make_async_remote_copy(src_ref=src, dst_ref=dst, send_sem=self.send_sem.at[b], recv_sem=sem.at[b],
                                     device_id={'tp': self.peers.at[bits]}, device_id_type=MESH).start()

    def own(self, b):
        mine = self.piece(b, self.peers.me)
        self.send(self.src.at[b], mine, b, self.rx, 2)
        self.send(self.src.at[b], mine, b, self.ry, 4)
        self.send(self.src.at[b], mine, b, self.rp, 1)

    def direct(self, b):
        half = self.seg // 2
        from_x, from_y = self.peers.at[2], self.peers.at[4]
        wait_bytes(self.piece(b, from_x), self.rx.at[b])
        first = self.piece(b, from_x, 0, half)
        self.send(first, first, b, self.rd0, 4)
        self.send(self.piece(b, from_x), self.piece(b, from_x), b, self.rp, 1)
        wait_bytes(self.piece(b, from_y), self.ry.at[b])
        second = self.piece(b, from_y, half, half)
        self.send(second, second, b, self.rd1, 2)
        self.send(self.piece(b, from_y), self.piece(b, from_y), b, self.rp, 1)

    def diagonal(self, b):
        half = self.seg // 2
        diag = self.peers.at[6]
        wait_bytes(self.piece(b, diag, 0, half), self.rd0.at[b])
        wait_bytes(self.piece(b, diag, half, half), self.rd1.at[b])
        self.send(self.piece(b, diag), self.piece(b, diag), b, self.rp, 1)

    def complete(self, b):
        wait_bytes(self.full.at[b, pl.ds(0, 4 * self.seg), :], self.rp.at[b])

    def load(self, b, slot, sem):
        for bits in range(8):
            t = self.peers.at[bits]
            src = self.src.at[b] if bits == 0 else self.piece(b, t)
            pltpu.make_async_copy(src, slot.at[pl.ds(pl.multiple_of(t * self.seg, self.seg), self.seg), :], sem).start()

    def drain(self, b):
        wait_bytes(self.full.at[b, pl.ds(0, 7 * self.seg), :], self.send_sem.at[b])


def project_kernel(y_loc, wq, wk, wv, bias, y_full, qk_out, v_out, st_out,
                   w_all, slot, qk_stage, v_stage, st_buf,
                   send_sem, rx, ry, rd0, rd1, rp, w_sem, load_sem, keep_sem, qk_sem, v_sem, st_send, st_recv):
    peers = Peers()
    me = peers.me
    rows, seg, _ = y_loc.shape
    cols = wq.shape[1]
    for n, w in enumerate((wq, wk, wv)):
        pltpu.make_async_copy(w, w_all.at[:, pl.ds(n * cols, cols)], w_sem.at[n]).start()
    entry_barrier(peers, range(1, 8))
    gather = RowGather(peers, y_loc, y_full, (send_sem, rx, ry, rd0, rd1, rp))
    for b in range(LOOKAHEAD):
        gather.own(b)
    for n, w in enumerate((wq, wk, wv)):
        pltpu.make_async_copy(w, w_all.at[:, pl.ds(n * cols, cols)], w_sem.at[n]).wait()

    def keep_copy(b):
        s = lax.rem(b, 2)
        return pltpu.make_async_copy(slot.at[s, pl.ds(pl.multiple_of(me * seg, seg), seg), :], gather.piece(b, me), keep_sem.at[s])

    def out_copies(b):
        s = lax.rem(b, 2)
        return (pltpu.make_async_copy(qk_stage.at[s], qk_out.at[b], qk_sem.at[s]),
                pltpu.make_async_copy(v_stage.at[s], v_out.at[b], v_sem.at[s]))

    def send_stats(b):
        for bits in range(1, 8):
            pltpu.make_async_remote_copy(src_ref=st_buf.at[me, b], dst_ref=st_buf.at[me, b], send_sem=st_send, recv_sem=st_recv,
                                         device_id={'tp': peers.at[bits]}, device_id_type=MESH).start()

    def compute(b):
        s = lax.rem(b, 2)
        wait_bytes(slot.at[s], load_sem.at[s])
        keep_copy(b).start()

        @pl.when(b >= 2)
        def _():
            for c in out_copies(b - 2):
                c.wait()

        tile = 256
        for m in range(slot.shape[1] // tile):
            block = pl.ds(m * tile, tile)
            acc = jnp.dot(slot[s, block, :], w_all[...], preferred_element_type=F32) + bias[...]
            qk_stage[s, block, :] = acc[:, :2 * cols]
            v_stage[s, block, :] = acc[:, 2 * cols:].astype(BF16)
        for j in range(slot.shape[1] // 128):
            for part in range(2):
                blk = qk_stage[s, pl.ds(j * 128, 128), pl.ds(part * cols, cols)]
                sq = blk * blk
                folded = sq[:, :128]
                for n in range(1, cols // 128):
                    folded = folded + sq[:, n * 128:(n + 1) * 128]
                st_buf[me, b, pl.ds(part * 4 + j, 1), :] = jnp.sum(folded.T, axis=0, keepdims=True)
        for c in out_copies(b):
            c.start()

    def step(i, carry):
        @pl.when(i + LOOKAHEAD < rows)
        def _():
            gather.own(i + LOOKAHEAD)

        @pl.when(i < rows)
        def _():
            gather.direct(i)

        @pl.when((i >= 1) & (i < rows + 1))
        def _():
            gather.diagonal(i - 1)

        @pl.when((i >= 2) & (i < rows + 2))
        def _():
            b = i - 2
            gather.complete(b)

            @pl.when(b >= 2)
            def _():
                keep_copy(b - 2).wait()

            gather.load(b, slot.at[lax.rem(b, 2)], load_sem.at[lax.rem(b, 2)])

        @pl.when((i >= 3) & (i < rows + 3))
        def _():
            compute(i - 3)

        @pl.when(i >= 4)
        def _():
            send_stats(i - 4)

        return carry

    lax.fori_loop(0, rows + 4, step, 0)
    for b in (rows - 2, rows - 1):
        for c in out_copies(b):
            c.wait()
        keep_copy(b).wait()

    def drain(b, carry):
        gather.drain(b)
        return carry

    lax.fori_loop(0, rows, drain, 0)
    wait_bytes(st_buf.at[pl.ds(0, 7)], st_send)
    wait_bytes(st_buf.at[pl.ds(0, 7)], st_recv)
    st_out[...] = jnp.sum(st_buf[...], axis=0)


def project(y_loc, w_q, w_k, w_v, bias):
    rows, seg, dim = y_loc.shape
    cols = w_q.shape[1]
    seq = seg * 8
    hbm = pl.BlockSpec(memory_space=pl.ANY)
    vmem = pl.BlockSpec(memory_space=pltpu.VMEM)
    dma = pltpu.SemaphoreType.DMA
    return pl.pallas_call(
        project_kernel,
        out_shape=(jax.ShapeDtypeStruct((rows, seq, dim), BF16), jax.ShapeDtypeStruct((rows, seq, 2 * cols), F32),
                   jax.ShapeDtypeStruct((rows, seq, cols), BF16), jax.ShapeDtypeStruct((rows, 8, 128), F32)),
        in_specs=[hbm, hbm, hbm, hbm, vmem],
        out_specs=(hbm, hbm, hbm, vmem),
        scratch_shapes=[pltpu.VMEM((dim, 3 * cols), BF16), pltpu.VMEM((2, seq, dim), BF16),
                        pltpu.VMEM((2, seq, 2 * cols), F32), pltpu.VMEM((2, seq, cols), BF16), pltpu.VMEM((8, rows, 8, 128), F32)]
        + [dma((rows,))] * 6 + [dma((3,)), dma((2,)), dma((2,)), dma((2,)), dma((2,)), dma, dma],
        compiler_params=pltpu.CompilerParams(collective_id=0, has_side_effects=True, vmem_limit_bytes=60 * 2**20),
        cost_estimate=pl.CostEstimate(flops=2 * rows * seq * dim * 3 * cols, bytes_accessed=4 * rows * seq * dim, transcendentals=0),
        name='gather_project',
    )(y_loc, w_q, w_k, w_v, bias)


def solution(mesh):
    tp_size = mesh.shape['tp']

    def device_step(x_loc, e_loc, m_block, w_q, b_q, w_k, b_k, w_v, b_v, w_o, b_o, g_q, g_k, pos_part, dy_loc):
        batch_size, seq_loc, model_dim = x_loc.shape
        seq_len = seq_loc * tp_size
        rows_all = batch_size * seq_len
        heads_loc = w_q.shape[1] // HEAD_DIM
        cols = w_q.shape[1]
        head_shape = (batch_size, seq_len, heads_loc, HEAD_DIM)
        cos_tab, sin_tab = rope_angles(pos_part)
        cos_bcast = cos_tab[None, :, None, :]
        sin_bcast = sin_tab[None, :, None, :]

        mod_rows = m_block[None] + e_loc
        shift_row = mod_rows[:, 0][:, None]
        scale_one = 1.0 + mod_rows[:, 1][:, None]
        gate_row = mod_rows[:, 2][:, None]
        x_float = x_loc.astype(jnp.float32)
        centered = x_float - jnp.mean(x_float, axis=-1, keepdims=True)
        inv_std = lax.rsqrt(jnp.mean(centered * centered, axis=-1, keepdims=True) + EPS_NORM)
        x_norm = centered * inv_std
        y_loc = (x_norm * scale_one + shift_row).astype(jnp.bfloat16)
        y_rows, qk_raw, v_rows, sq_parts = project(y_loc, w_q, w_k, w_v, jnp.concatenate([b_q, b_k, b_v])[None])
        y_full = y_rows.reshape(rows_all, model_dim)
        q_raw = qk_raw[:, :, :cols].reshape(rows_all, cols)
        k_raw = qk_raw[:, :, cols:].reshape(rows_all, cols)
        v_heads = v_rows.reshape(head_shape)
        sq_sums = jnp.moveaxis(sq_parts.reshape(batch_size, 2, seq_len), 1, 0).reshape(2, rows_all)

        inv_rms = lax.rsqrt(sq_sums / model_dim + EPS_NORM)[:, :, None]
        q_hat = q_raw * inv_rms[0]
        k_hat = k_raw * inv_rms[1]
        q_rot = rope_rotate((q_hat * g_q).reshape(head_shape), cos_bcast, sin_bcast).astype(jnp.bfloat16)
        k_rot = rope_rotate((k_hat * g_k).reshape(head_shape), cos_bcast, sin_bcast).astype(jnp.bfloat16)
        attn_out, attn_pull = jax.vjp(attend, q_rot, k_rot, v_heads)
        o_flat = attn_out.reshape(rows_all, heads_loc * HEAD_DIM)
        part_sum = jnp.dot(o_flat, w_o, preferred_element_type=jnp.float32).astype(jnp.bfloat16).reshape(batch_size, seq_len, model_dim)
        proj_loc = lax.psum_scatter(part_sum, 'tp', scatter_dimension=1, tiled=True).astype(jnp.float32) + b_o
        x_out = (x_float + gate_row * proj_loc).astype(jnp.bfloat16)

        dy_float = dy_loc.astype(jnp.float32)
        d_gate = jnp.sum(dy_float * proj_loc, axis=1)
        d_proj = lax.all_gather((dy_float * gate_row).astype(jnp.bfloat16), 'tp', axis=1, tiled=True).reshape(rows_all, model_dim)
        d_wo = lax.dot_general(o_flat, d_proj, ROW_CONTRACT, preferred_element_type=jnp.float32).astype(jnp.bfloat16)
        d_attn = lax.dot_general(d_proj, w_o, COL_CONTRACT, preferred_element_type=jnp.float32).astype(jnp.bfloat16).reshape(head_shape)
        dq_rot, dk_rot, dv_heads = attn_pull(d_attn)
        dq_hat = rope_rotate(dq_rot.astype(jnp.float32), cos_bcast, -sin_bcast).reshape(rows_all, -1)
        dk_hat = rope_rotate(dk_rot.astype(jnp.float32), cos_bcast, -sin_bcast).reshape(rows_all, -1)
        d_gq = jnp.sum(dq_hat * q_hat, axis=0)
        d_gk = jnp.sum(dk_hat * k_hat, axis=0)
        dq_scaled = dq_hat * g_q
        dk_scaled = dk_hat * g_k
        stat_grads = lax.psum(jnp.stack([jnp.sum(dq_scaled * q_hat, axis=-1), jnp.sum(dk_scaled * k_hat, axis=-1)]), 'tp')[:, :, None] / model_dim
        dq_raw = (inv_rms[0] * (dq_scaled - q_hat * stat_grads[0])).astype(jnp.bfloat16)
        dk_raw = (inv_rms[1] * (dk_scaled - k_hat * stat_grads[1])).astype(jnp.bfloat16)
        dv_flat = dv_heads.reshape(rows_all, -1)
        d_wq = lax.dot_general(y_full, dq_raw, ROW_CONTRACT, preferred_element_type=jnp.float32).astype(jnp.bfloat16)
        d_wk = lax.dot_general(y_full, dk_raw, ROW_CONTRACT, preferred_element_type=jnp.float32).astype(jnp.bfloat16)
        d_wv = lax.dot_general(y_full, dv_flat, ROW_CONTRACT, preferred_element_type=jnp.float32).astype(jnp.bfloat16)
        dy_part = (lax.dot_general(dq_raw, w_q, COL_CONTRACT, preferred_element_type=jnp.float32)
                   + lax.dot_general(dk_raw, w_k, COL_CONTRACT, preferred_element_type=jnp.float32)
                   + lax.dot_general(dv_flat, w_v, COL_CONTRACT, preferred_element_type=jnp.float32))
        dy_part = dy_part.astype(jnp.bfloat16).reshape(batch_size, seq_len, model_dim)
        d_y = lax.psum_scatter(dy_part, 'tp', scatter_dimension=1, tiled=True).astype(jnp.float32)
        d_mod = lax.psum(jnp.stack([jnp.sum(d_y, axis=1), jnp.sum(d_y * x_norm, axis=1), d_gate], axis=1), 'tp')
        d_norm = d_y * scale_one
        d_x = dy_float + inv_std * (d_norm - jnp.mean(d_norm, axis=-1, keepdims=True) - x_norm * jnp.mean(d_norm * x_norm, axis=-1, keepdims=True))
        return (x_out, d_x.astype(jnp.bfloat16), d_mod, jnp.sum(d_mod, axis=0), d_wq, d_wk, d_wv, d_wo, d_gq, d_gk)

    in_specs = (P('dp', 'tp', None), P('dp', None, None), P(None, None), P(None, 'tp'), P('tp'), P(None, 'tp'), P('tp'),
                P(None, 'tp'), P('tp'), P('tp', None), P(None), P('tp'), P('tp'), P('dp', None), P('dp', 'tp', None))
    out_specs = (P('dp', 'tp', None), P('dp', 'tp', None), P('dp', None, None), P('dp', None), P('dp', 'tp'), P('dp', 'tp'),
                 P('dp', 'tp'), P(('dp', 'tp'), None), P(('dp', 'tp')), P(('dp', 'tp')))
    return jax.shard_map(device_step, mesh=mesh, in_specs=in_specs, out_specs=out_specs, check_vma=False)
```

```python
import functools

import jax
import jax.numpy as jnp
from jax import lax
from jax.experimental import pallas as pl
from jax.experimental.pallas import tpu as pltpu
from jax.sharding import PartitionSpec as P

HEAD_DIM = 128
EPS_NORM = 1e-6
ROPE_BASE = 10000.0
ROW_CONTRACT = (((0,), (0,)), ((), ()))
COL_CONTRACT = (((1,), (1,)), ((), ()))
MESH = pl.DeviceIdType.MESH
F32 = jnp.float32
BF16 = jnp.bfloat16
PARTS = 8
PANEL = 1024
EARLY = 12
VMEM_ALL = 67043328
SCORE_SCALE = HEAD_DIM ** -0.5 * 1.4426950408889634


def rope_angles(positions):
    half_dim = HEAD_DIM // 2
    side_len = HEAD_DIM // 6
    first_len = half_dim - 2 * side_len
    pair_idx = jnp.arange(half_dim)
    section = (pair_idx >= first_len).astype(jnp.int32) + (pair_idx >= first_len + side_len).astype(jnp.int32)
    offset = jnp.where(section == 0, 0, jnp.where(section == 1, first_len, first_len + side_len))
    sec_width = jnp.where(section == 0, first_len, side_len)
    freq_vals = ROPE_BASE ** (-(pair_idx - offset).astype(jnp.float32) / sec_width.astype(jnp.float32))
    select = jnp.where(section[None, :] == jnp.arange(3)[:, None], freq_vals[None, :], 0.0)
    angles = jnp.sum(positions.astype(jnp.float32)[:, :, None] * select[None, :, :], axis=1)
    return jnp.cos(angles), jnp.sin(angles)


def rope_tables(positions):
    cos_tab, sin_tab = (jnp.repeat(t, 2, axis=1) for t in rope_angles(positions))
    even = (jnp.arange(HEAD_DIM) % 2 == 0)[None]
    up = jnp.where(even, -sin_tab, 0.0)
    down = jnp.where(even, 0.0, sin_tab)
    scale = HEAD_DIM ** -0.5
    return jnp.stack([cos_tab, up, down, cos_tab * scale, -up * scale, -down * scale])


class Peers:
    def __init__(self):
        me = lax.axis_index('tp')
        self.me = me
        core, col, row = lax.rem(me, 2), lax.rem(me // 2, 2), me // 4

        def flip(bits):
            out = me
            if bits & 1:
                out = out + 1 - 2 * core
            if bits & 2:
                out = out + 2 - 4 * col
            if bits & 4:
                out = out + 4 - 8 * row
            return out

        self.at = [flip(bits) for bits in range(PARTS)]
        self.partner, self.x, self.y, self.diag = (self.at[bits] for bits in (1, 2, 4, 6))


def entry_barrier(peers, which):
    barrier = pltpu.get_barrier_semaphore()
    for bits in which:
        pl.semaphore_signal(barrier, inc=1, device_id={'tp': peers.at[bits]}, device_id_type=MESH)
    pl.semaphore_wait(barrier, len(which))


def wait_local(ref, sem):
    pltpu.make_async_copy(ref, ref, sem).wait()


def wait_bytes(ref, sem):
    pltpu.make_async_copy(ref, ref, sem).wait()


def even(b):
    return lax.rem(b, 2)


class RowGather:
    def __init__(self, peers, src, full, sems, seg):
        self.peers, self.src, self.full, self.seg = peers, src, full, seg
        self.send_sem, self.rx, self.ry, self.rd0, self.rd1, self.rp = sems
        self.lower, self.upper = (0, seg // 2), (seg // 2, seg // 2)

    def piece(self, b, t, part=None):
        lo, n = part or (0, self.seg)
        return self.full.at[b, pl.ds(pl.multiple_of(t * self.seg + lo, 32), n), :]

    def first(self, b, pieces):
        return self.full.at[b, pl.ds(0, pieces * self.seg), :]

    def send(self, src, dst, b, sem, t):
        pltpu.make_async_remote_copy(src_ref=src, dst_ref=dst, send_sem=self.send_sem.at[b], recv_sem=sem.at[b],
                                     device_id={'tp': t}, device_id_type=MESH).start()

    def own(self, b):
        p = self.peers
        for sem, t in ((self.rx, p.x), (self.ry, p.y), (self.rp, p.partner)):
            self.send(self.src(b), self.piece(b, p.me), b, sem, t)

    def direct(self, b):
        p = self.peers
        for near, sem, part, diag_sem, far in ((p.x, self.rx, self.lower, self.rd0, p.y), (p.y, self.ry, self.upper, self.rd1, p.x)):
            whole, some = self.piece(b, near), self.piece(b, near, part)
            wait_bytes(whole, sem.at[b])
            self.send(some, some, b, diag_sem, far)
            self.send(whole, whole, b, self.rp, p.partner)

    def diagonal(self, b):
        p = self.peers
        wait_bytes(self.piece(b, p.diag, self.lower), self.rd0.at[b])
        wait_bytes(self.piece(b, p.diag, self.upper), self.rd1.at[b])
        self.send(self.piece(b, p.diag), self.piece(b, p.diag), b, self.rp, p.partner)

    def complete(self, b):
        wait_bytes(self.first(b, 4), self.rp.at[b])

    def load(self, b, slot, sem):
        for n, t in enumerate(self.peers.at):
            src = self.piece(b, t) if n else self.src(b)
            pltpu.make_async_copy(src, slot.at[pl.ds(pl.multiple_of(t * self.seg, self.seg), self.seg), :], sem).start()

    def drain(self, b):
        wait_bytes(self.first(b, PARTS - 1), self.send_sem.at[b])


def stage_of(i, lag, count, work):
    @pl.when((i >= lag) & (i < count + lag))
    def _():
        work(i - lag)


def attend_kernel(y_loc, dp_loc, wq, wk, wv, bias, gains, tabs, wo,
                  y_full, dp_full, dqkv_out, o_tok, wo_full, dwo_out, pair_in, pair_out, half_out, dg_out,
                  w_all, y_slot, d_slot, qk_ring, v_ring, rot, o_stage, datt, dqk, dqs, dqkv_stage, col_inv, p_buf, ds_buf,
                  dwo_acc, stage, pair_stage, pair_buf, norm_buf, stat_buf,
                  y_sems, d_sems, wo_sems, w_sem, y_sem, d_sem, keep_sem, norm_send, norm_recv, stat_send, stat_recv,
                  o_send, o_keep, o_recv, out_sem, pair_send, pair_recv, pair_load, pair_sem, wo_keep, z_send, z_recv, dwo_sem, half_send, half_recv):
    peers = Peers()
    me = peers.me
    depth = lax.axis_index('dp')
    rows, seg, dim = y_loc.shape
    seq = seg * PARTS
    cols = wq.shape[1]
    heads = cols // HEAD_DIM
    blk = HEAD_DIM
    blocks = seq // blk
    wide = 2 * cols
    hemi = dim // 2
    weights = [pltpu.make_async_copy(w, w_all.at[:, pl.ds(n * cols, cols)], w_sem.at[n]) for n, w in enumerate((wq, wk, wv))]
    for c in weights:
        c.start()
    barrier = pltpu.get_barrier_semaphore()
    for t in peers.at[1:]:
        pl.semaphore_signal(barrier, inc=1, device_id={'tp': t}, device_id_type=MESH)
    pl.semaphore_signal(barrier, inc=1, device_id={'dp': 1 - depth}, device_id_type=MESH)
    pl.semaphore_wait(barrier, PARTS)
    gy = RowGather(peers, lambda b: y_loc.at[b], y_full, y_sems, seg)
    gd = RowGather(peers, lambda b: dp_loc.at[b], dp_full, d_sems, seg)
    gw = RowGather(peers, lambda b: wo.at[:, pl.ds(pl.multiple_of(b * hemi, HEAD_DIM), hemi)], wo_full, wo_sems, cols)
    gy.own(0)
    gd.own(0)
    gy.own(1)
    dwo_acc[...] = jnp.zeros_like(dwo_acc)
    dg_out[...] = jnp.zeros_like(dg_out)
    for c in weights:
        c.wait()

    def mine(b, width):
        return pl.ds(pl.multiple_of(b * width, width), width)

    keep_y = pltpu.make_async_copy(y_slot.at[mine(me, seg), :], gy.piece(0, me), keep_sem)

    def out_copy(b):
        return pltpu.make_async_copy(dqkv_stage.at[even(b)], dqkv_out.at[b], out_sem.at[even(b)])

    def pair_copy(b):
        return pltpu.make_async_copy(pair_stage.at[even(b)], pair_out.at[b], pair_sem.at[even(b)])

    def o_rows(b, t):
        return o_stage.at[even(b), mine(t, seg), :]

    def keep_o(b):
        return pltpu.make_async_copy(o_rows(b, me), o_tok.at[b, :, mine(me, cols)], o_keep.at[even(b)])

    def keep_wo(h):
        return pltpu.make_async_copy(gw.src(h), wo_full.at[h, mine(me, cols), :], wo_keep.at[h])

    def remote(src, dst, send, recv, device):
        return pltpu.make_async_remote_copy(src_ref=src, dst_ref=dst, send_sem=send, recv_sem=recv, device_id=device, device_id_type=MESH)

    def send_sums(b, buf, send, recv):
        for t in peers.at[1:]:
            remote(buf.at[me, b], buf.at[me, b], send, recv.at[b], {'tp': t}).start()

    def send_row(b):
        send_sums(b, stat_buf, stat_send, stat_recv)
        for t in peers.at[1:]:
            remote(o_rows(b, t), o_tok.at[b, :, mine(me, cols)], o_send.at[even(b)], o_recv, {'tp': t}).start()
        keep_o(b).start()

    def wait_row_sent(b):
        wait_bytes(o_stage.at[even(b), pl.ds(0, seq - seg), :], o_send.at[even(b)])
        keep_o(b).wait()

    def pair_sends(b):
        for n in range(4):
            t = peers.at[1 ^ (2 * n)]
            remote(stage.at[mine(t, seg), :], pair_in.at[b, n], pair_send, pair_recv.at[b], {'tp': peers.at[1]}).start()

    def spread(row):
        return jnp.broadcast_to(row, (blk, blk)).T

    def turned(x, sl, kind):
        c, up, down = tabs[kind, sl, :], tabs[kind + 1, sl, :], tabs[kind + 2, sl, :]
        return x * c + pltpu.roll(x, HEAD_DIM - 1, 1) * up + pltpu.roll(x, 1, 1) * down

    def lane_cols(part, h):
        return pl.ds(part * cols + h * HEAD_DIM, HEAD_DIM)

    def load_y(b):
        gy.complete(b)

        @pl.when(b >= 1)
        def _():
            keep_y.wait()

        gy.load(b, y_slot, y_sem)

    def load_d(b):
        gd.complete(b)
        gd.load(b, d_slot.at[even(b)], d_sem.at[even(b)])

    def qkv(b):
        ring = lax.rem(b, 4)
        wait_local(y_slot, y_sem)
        pltpu.make_async_copy(y_slot.at[mine(me, seg), :], gy.piece(b, me), keep_sem).start()
        tile = 2 * blk
        for m in range(seq // tile):
            sl = pl.ds(m * tile, tile)
            acc = jnp.dot(y_slot[sl, :], w_all[...], preferred_element_type=F32) + bias[...]
            qk_ring[ring, sl, :] = acc[:, :wide]
            v_ring[even(b), sl, :] = acc[:, wide:].astype(BF16)
        for j in range(blocks):
            for part in range(2):
                total = None
                for h in range(heads):
                    x = qk_ring[ring, pl.ds(j * blk, blk), lane_cols(part, h)]
                    total = x * x if total is None else total + x * x
                norm_buf[me, b, pl.ds(part * blocks + j, 1), :] = jnp.sum(total.T, axis=0, keepdims=True)

    def inv_norms(b):
        return lax.rsqrt(jnp.sum(norm_buf[:, b], axis=0) * (1.0 / dim) + EPS_NORM)

    def attend(b):
        s, ring = even(b), lax.rem(b, 4)
        wait_bytes(norm_buf.at[pl.ds(0, PARTS - 1), b], norm_recv.at[b])
        wait_local(d_slot.at[s], d_sem.at[s])

        @pl.when(b >= 2)
        def _():
            wait_row_sent(b - 2)
            out_copy(b - 2).wait()

        tile = 2 * blk
        for m in range(seq // tile):
            sl = pl.ds(m * tile, tile)
            datt[sl, :] = lax.dot_general(d_slot[s, sl, :], wo[...], COL_CONTRACT, preferred_element_type=F32).astype(BF16)

        inv = inv_norms(b)
        for j in range(blocks):
            sl = pl.ds(j * blk, blk)
            for part in range(2):
                row = part * blocks + j
                scale = spread(inv[row:row + 1, :])
                col_inv[s, part, sl, :] = scale
                for h in range(heads):
                    cs = lane_cols(part, h)
                    rot[sl, cs] = turned(qk_ring[ring, sl, cs] * scale * gains[:, cs], sl, 0).astype(BF16)

        def head(h, carry):
            hq, hk, hv = (pl.ds(pl.multiple_of(n * cols + h * HEAD_DIM, HEAD_DIM), HEAD_DIM) for n in range(3))
            k_h, v_h = rot[:, hk], v_ring[s, :, hq]
            for j in range(blocks):
                sl = pl.ds(j * blk, blk)
                sc = lax.dot_general(rot[sl, hq], k_h, COL_CONTRACT, preferred_element_type=F32) * SCORE_SCALE
                p = jnp.exp2(sc - jnp.max(sc, axis=-1, keepdims=True))
                p = p * (1.0 / jnp.sum(p, axis=-1, keepdims=True))
                pb = p.astype(BF16)
                p_buf[sl, :] = pb
                o_stage[s, sl, hq] = jnp.dot(pb, v_h, preferred_element_type=F32).astype(BF16)
                dp = lax.dot_general(datt[sl, hq], v_h, COL_CONTRACT, preferred_element_type=F32)
                ds = (p * (dp - jnp.sum(p * dp, axis=-1, keepdims=True))).astype(BF16)
                ds_buf[sl, :] = ds
                dqk[sl, hq] = jnp.dot(ds, k_h, preferred_element_type=F32)
            dqk[:, hk] = lax.dot_general(ds_buf[...], rot[:, hq], ROW_CONTRACT, preferred_element_type=F32)
            dqkv_stage[s, :, hv] = lax.dot_general(p_buf[...], datt[:, hq], ROW_CONTRACT, preferred_element_type=F32).astype(BF16)
            return carry

        lax.fori_loop(0, heads, head, 0)

        for j in range(blocks):
            sl = pl.ds(j * blk, blk)
            for part in range(2):
                scale = col_inv[s, part, sl, :]
                total = None
                for h in range(heads):
                    cs = lane_cols(part, h)
                    dx = turned(dqk[sl, cs], sl, 3)
                    prod = dx * (qk_ring[ring, sl, cs] * scale)
                    dg_out[:, cs] = dg_out[:, cs] + jnp.sum(prod, axis=0, keepdims=True)
                    dqs[s, sl, cs] = dx * gains[:, cs]
                    prod = prod * gains[:, cs]
                    total = prod if total is None else total + prod
                stat_buf[me, b, pl.ds(part * blocks + j, 1), :] = jnp.sum(total.T, axis=0, keepdims=True)

        for n in range(3):
            cs = pl.ds(n * PANEL, PANEL)
            dwo_acc[:, cs] += lax.dot_general(o_stage[s], d_slot[s, :, cs], ROW_CONTRACT, preferred_element_type=F32)

    def finish(b):
        s, ring = even(b), lax.rem(b, 4)
        wait_bytes(stat_buf.at[pl.ds(0, PARTS - 1), b], stat_recv.at[b])
        inv = inv_norms(b)
        coef = jnp.sum(stat_buf[:, b], axis=0) * (1.0 / dim) * inv * inv
        for j in range(blocks):
            sl = pl.ds(j * blk, blk)
            for part in range(2):
                row = part * blocks + j
                scale = col_inv[s, part, sl, :]
                pull = spread(coef[row:row + 1, :])
                for h in range(heads):
                    cs = lane_cols(part, h)
                    dqkv_stage[s, sl, cs] = (scale * dqs[s, sl, cs] - pull * qk_ring[ring, sl, cs]).astype(BF16)
        out_copy(b).start()
        for n in range(3):
            cs = pl.ds(n * PANEL, PANEL)
            stage[:, cs] = lax.dot_general(dqkv_stage[s], w_all[cs, :], COL_CONTRACT, preferred_element_type=F32).astype(BF16)

    def pair_sum(b):
        wait_bytes(pair_in.at[b], pair_recv.at[b])
        load = pltpu.make_async_copy(pair_in.at[b], pair_buf, pair_load)
        load.start()

        @pl.when(b >= 1)
        def _():
            pair_copy(b - 1).wait()

        wait_bytes(pair_in.at[b], pair_send)
        load.wait()
        for n in range(4):
            pair_stage[even(b), n] = (stage[mine(peers.at[2 * n], seg), :].astype(F32) + pair_buf[n].astype(F32)).astype(BF16)
        pair_copy(b).start()

    def spread_wo(h):
        gw.complete(h)
        for t in peers.at[1:]:
            piece = gw.piece(h, t)
            remote(piece, piece, z_send, z_recv, {'dp': 1 - depth}).start()

    def half_sends(b):
        for n, t in enumerate((peers.y, peers.x)):
            remote(pair_out.at[b, 3, mine(n, seg // 2), :], half_out.at[b, n], half_send.at[b], half_recv.at[n, b], {'tp': t}).start()

    def early_halves(lo, hi):
        def work(b):
            for n in range(lo, hi):
                half_sends(n)
        return work

    def step(i, carry):
        stage_of(i, 4, rows, send_row)
        stage_of(i, rows, 1, early_halves(0, 3))
        stage_of(i, rows + 1, 1, early_halves(6, 9))
        stage_of(i, rows + 2, 1, early_halves(9, 11))
        stage_of(i, rows + 3, 1, early_halves(11, EARLY))
        stage_of(i + 1, 1, rows - 1, lambda b: gd.own(b + 1))
        stage_of(i, 0, rows, gy.direct)
        stage_of(i, 1, rows, gy.diagonal)
        stage_of(i, 2, rows, load_d)
        stage_of(i, 2, 1, lambda b: gw.own(depth))
        stage_of(i, 4, 1, lambda b: gw.direct(depth))
        stage_of(i, 5, 1, lambda b: gw.diagonal(depth))
        stage_of(i, 6, 1, lambda b: spread_wo(depth))
        stage_of(i, 2, rows, qkv)
        stage_of(i, 6, rows, pair_sum)
        stage_of(i, 5, rows, finish)
        stage_of(i, 2, rows, lambda b: send_sums(b, norm_buf, norm_send, norm_recv))
        stage_of(i, 5, rows, pair_sends)
        stage_of(i, rows, 1, early_halves(3, 6))
        stage_of(i + 2, 2, rows - 2, lambda b: gy.own(b + 2))
        stage_of(i, 0, rows, gd.direct)
        stage_of(i, 1, rows, gd.diagonal)
        stage_of(i, 1, rows, load_y)
        stage_of(i, 3, rows, attend)
        return carry

    keep_wo(0).start()
    keep_wo(1).start()
    lax.fori_loop(0, rows + 6, step, 0)
    stage[pl.ds(0, cols), :] = dwo_acc[...].astype(BF16)
    dwo_copy = pltpu.make_async_copy(stage.at[pl.ds(0, cols), :], dwo_out, dwo_sem)
    dwo_copy.start()
    keep_y.wait()
    keep_wo(0).wait()
    keep_wo(1).wait()
    for b in (rows - 2, rows - 1):
        wait_row_sent(b)
        out_copy(b).wait()
    pair_copy(rows - 1).wait()

    def drain(b, carry):
        gy.drain(b)
        gd.drain(b)
        return carry

    lax.fori_loop(0, rows, drain, 0)
    gw.drain(depth)
    others = pl.ds(0, PARTS - 1)
    for buf, sem in ((norm_buf, norm_send), (stat_buf, stat_send)):
        wait_bytes(buf.at[others], sem)
    wait_bytes(o_tok.at[pl.ds(0, rows - rows // PARTS)], o_recv)
    sent = wo_full.at[0, pl.ds(0, dim - cols), :]
    wait_bytes(sent, z_send)
    wait_bytes(sent, z_recv)
    dwo_copy.wait()
    for b in range(EARLY):
        wait_bytes(half_out.at[b], half_send.at[b])
        for n in range(2):
            wait_bytes(half_out.at[b, n], half_recv.at[n, b])


def attend_grad(y_loc, dp_loc, w_q, w_k, w_v, bias, gains, tabs, w_o):
    rows, seg, dim = y_loc.shape
    cols = w_o.shape[0]
    seq = seg * PARTS
    hbm = pl.BlockSpec(memory_space=pl.ANY)
    vmem = pl.BlockSpec(memory_space=pltpu.VMEM)
    dma = pltpu.SemaphoreType.DMA
    two, each = dma((2,)), dma((rows,))
    gathered = jax.ShapeDtypeStruct((rows, seq, dim), BF16)
    paired = jax.ShapeDtypeStruct((rows, 4, seg, dim), BF16)
    wide, all_cols = 2 * cols, 3 * cols
    return pl.pallas_call(
        attend_kernel,
        out_shape=(gathered, gathered, jax.ShapeDtypeStruct((rows, seq, all_cols), BF16), jax.ShapeDtypeStruct((rows, seg, dim), BF16),
                   jax.ShapeDtypeStruct((2, dim, dim // 2), BF16), jax.ShapeDtypeStruct((cols, dim), BF16), paired, paired,
                   jax.ShapeDtypeStruct((EARLY, 2, seg // 2, dim), BF16),
                   jax.ShapeDtypeStruct((1, wide), F32)),
        in_specs=[hbm] * 5 + [vmem] * 4,
        out_specs=[hbm] * 9 + [vmem],
        scratch_shapes=[pltpu.VMEM((dim, all_cols), BF16), pltpu.VMEM((seq, dim), BF16), pltpu.VMEM((2, seq, dim), BF16),
                        pltpu.VMEM((4, seq, wide), F32), pltpu.VMEM((2, seq, cols), BF16), pltpu.VMEM((seq, wide), BF16),
                        pltpu.VMEM((2, seq, cols), BF16), pltpu.VMEM((seq, cols), BF16), pltpu.VMEM((seq, wide), F32),
                        pltpu.VMEM((2, seq, wide), F32), pltpu.VMEM((2, seq, all_cols), BF16), pltpu.VMEM((2, 2, seq, HEAD_DIM), F32),
                        pltpu.VMEM((seq, seq), BF16), pltpu.VMEM((seq, seq), BF16), pltpu.VMEM((cols, dim), F32), pltpu.VMEM((seq, dim), BF16),
                        pltpu.VMEM((2, 4, seg, dim), BF16), pltpu.VMEM((4, seg, dim), BF16),
                        pltpu.VMEM((PARTS, rows, 8, HEAD_DIM), F32), pltpu.VMEM((PARTS, rows, 8, HEAD_DIM), F32)]
        + [[each] * 6, [each] * 6, [two] * 6, dma((3,)), dma, two, dma, dma, each, dma, each,
           two, two, dma, two, dma, each, dma, two, two, dma, dma, dma, dma((EARLY,)), dma((2, EARLY))],
        compiler_params=pltpu.CompilerParams(collective_id=0, has_side_effects=True, vmem_limit_bytes=VMEM_ALL),
        name='gather_attend',
    )(y_loc, dp_loc, w_q, w_k, w_v, bias, gains, tabs, w_o)


def scatter_kernel(pairs, halves, dqkv, y_full, o_tok, wo_full, x_loc, d_out, scale_rows, gate_rows, b_o,
                   xo_out, dx_out, mod_out, dw_out, half_in, last_in,
                   dt_slot, y_slot, dq_turned, half_stage, half_buf, last_buf, dw_acc,
                   o_all, x_all, dy_all, w_slot, proj, xo_stage, dx_stage, sums, mod_part, mod_in,
                   dt_sem, y_sem, half_send, last_send, half_recv0, half_recv1, last_recv0, last_recv1, half_load, last_load, dw_sem,
                   all_sem, wch_sem, xo_sem, dx_sem, part_send, part_recv, mod_send, mod_recv):
    peers = Peers()
    me = peers.me
    rows, seq, dim = y_full.shape
    seg = seq // PARTS
    half = seg // 2
    cols = dim // PARTS
    width = w_slot.shape[2]
    chunks = dim // width
    group = mod_part.shape[2]
    every = [pltpu.make_async_copy(src, dst, all_sem.at[n]) for n, (src, dst) in enumerate(((o_tok, o_all), (x_loc, x_all), (d_out, dy_all)))]

    def mine(b, size):
        return pl.ds(pl.multiple_of(b * size, size), size)

    def dt_copy(b):
        return pltpu.make_async_copy(dqkv.at[b], dt_slot.at[even(b)], dt_sem.at[even(b)])

    def y_copy(b):
        return pltpu.make_async_copy(y_full.at[b], y_slot.at[even(b)], y_sem.at[even(b)])

    def dx_copy(b):
        return pltpu.make_async_copy(dx_stage.at[even(b)], dx_out.at[b], dx_sem.at[even(b)])

    def chunk_copy(n):
        per = chunks // 2
        return pltpu.make_async_copy(wo_full.at[n // per, :, mine(lax.rem(n, per), width)], w_slot.at[even(n)], wch_sem.at[even(n)])

    def xo_copy(n):
        return pltpu.make_async_copy(xo_stage.at[even(n)], xo_out.at[:, :, mine(n, width)], xo_sem.at[even(n)])

    def remote(src, dst, send, recv, t):
        pltpu.make_async_remote_copy(src_ref=src, dst_ref=dst, send_sem=send, recv_sem=recv,
                                     device_id={'tp': t}, device_id_type=MESH).start()

    def half_sends(b):
        remote(pairs.at[b, 3, pl.ds(0, half), :], half_in.at[b, 0], half_send.at[b], half_recv0.at[b], peers.y)
        remote(pairs.at[b, 3, pl.ds(half, half), :], half_in.at[b, 1], half_send.at[b], half_recv1.at[b], peers.x)

    ring = half_stage.shape[0]

    def last_sends(b):
        s = lax.rem(b, ring)
        remote(half_stage.at[s, 0], last_in.at[b, 0], last_send.at[b], last_recv0.at[b], peers.x)
        remote(half_stage.at[s, 1], last_in.at[b, 1], last_send.at[b], last_recv1.at[b], peers.y)

    def half_loads(b, source=None):
        s = even(b)
        return (pltpu.make_async_copy((half_in if source is None else source).at[b], half_buf.at[s], half_load.at[0, s]),
                pltpu.make_async_copy(pairs.at[b, pl.ds(1, 2)], half_stage.at[lax.rem(b, ring)], half_load.at[1, s]))

    def last_loads(b):
        return (pltpu.make_async_copy(last_in.at[b], last_buf.at[pl.ds(0, 2)], last_load.at[0]),
                pltpu.make_async_copy(pairs.at[b, 0], last_buf.at[2], last_load.at[1]))

    def fetch_half(b):
        @pl.when(b >= ring)
        def _():
            wait_bytes(last_in.at[b - ring], last_send.at[b - ring])

        @pl.when(b < EARLY)
        def _():
            for c in half_loads(b, halves):
                c.start()

        @pl.when(b >= EARLY)
        def _():
            wait_bytes(half_in.at[b, 0], half_recv0.at[b])
            wait_bytes(half_in.at[b, 1], half_recv1.at[b])
            for c in half_loads(b):
                c.start()

    def half_sum(b):
        s, r = even(b), lax.rem(b, ring)
        for c in half_loads(b):
            c.wait()
        for n in range(2):
            sl = pl.ds(n * half, half)
            half_stage[r, n, sl, :] = (half_stage[r, n, sl, :].astype(F32) + half_buf[s, n].astype(F32)).astype(BF16)

    def fetch_last(b):
        wait_bytes(last_in.at[b, 0], last_recv0.at[b])
        wait_bytes(last_in.at[b, 1], last_recv1.at[b])
        for c in last_loads(b):
            c.start()

    def last_sum(b):
        for c in last_loads(b):
            c.wait()

        @pl.when(b >= 2)
        def _():
            dx_copy(b - 2).wait()

        sums[...] = jnp.zeros_like(sums)
        scale = scale_rows[pl.ds(b, 1), :]
        few = 16

        def tokens(n, carry):
            sl = mine(n, few)
            dy = last_buf[2, sl, :].astype(F32) + last_buf[0, sl, :].astype(F32) + last_buf[1, sl, :].astype(F32)
            x = x_all[b, sl, :].astype(F32)
            x = x - jnp.mean(x, axis=-1, keepdims=True)
            inv_std = lax.rsqrt(jnp.mean(x * x, axis=-1, keepdims=True) + EPS_NORM)
            x = x * inv_std
            sums[0] += dy
            sums[1] += dy * x
            dn = dy * scale
            pull = x * jnp.mean(dn * x, axis=-1, keepdims=True) + jnp.mean(dn, axis=-1, keepdims=True)
            dx_stage[even(b), sl, :] = (dy_all[b, sl, :].astype(F32) + inv_std * (dn - pull)).astype(BF16)
            return carry

        lax.fori_loop(0, seg // few, tokens, 0)
        dx_copy(b).start()
        for n in range(2):
            mod_part[b // group, n, pl.ds(lax.rem(b, group), 1), :] = jnp.sum(sums[n], axis=0, keepdims=True)

    def project_out(n):
        cs = mine(n, width)

        @pl.when(n == 0)
        def _():
            for c in every:
                c.wait()

        @pl.when(n >= 2)
        def _():
            xo_copy(n - 2).wait()

        chunk_copy(n).wait()
        flat = o_all[...].reshape(rows * seg, dim)
        proj[...] = (jnp.dot(flat, w_slot[even(n)], preferred_element_type=F32) + b_o[:, cs]).reshape(proj.shape)

        def row(b, carry):
            out = proj[b]
            xo_stage[even(n), b] = (x_all[b, :, cs].astype(F32) + gate_rows[pl.ds(b, 1), cs] * out).astype(BF16)
            mod_part[b // group, 2, pl.ds(lax.rem(b, group), 1), cs] = jnp.sum(dy_all[b, :, cs].astype(F32) * out, axis=0, keepdims=True)
            return carry

        lax.fori_loop(0, rows, row, 0)
        xo_copy(n).start()

        @pl.when(n + 2 < chunks)
        def _():
            chunk_copy(n + 2).start()

    def fetch_row(b):
        y_copy(b).start()
        dt_copy(b).start()

    def weight_grad(b):
        s = even(b)
        y_copy(b).wait()
        dt_copy(b).wait()
        dq_turned[...] = dt_slot[s].T
        for n in range(6):
            cs = pl.ds(n * (PANEL // 2), PANEL // 2)
            dw_acc[:, cs] += jnp.dot(dq_turned[...], y_slot[s, :, cs], preferred_element_type=F32)

    def share_parts(g):
        for t in peers.at[1:]:
            remote(mod_part.at[g, :, :, mine(t, cols)], mod_in.at[g, me], part_send.at[g], part_recv.at[g], t)
        mod_in[g, me] = mod_part[g, :, :, mine(me, cols)]

    def merge_parts(g):
        wait_bytes(mod_in.at[g, pl.ds(0, PARTS - 1)], part_recv.at[g])
        mod_out[g, :, :, mine(me, cols)] = jnp.sum(mod_in[g], axis=0)

    def share_mods(g):
        here = mod_out.at[g, :, :, mine(me, cols)]
        for t in peers.at[1:]:
            remote(here, here, mod_send.at[g], mod_recv.at[g], t)

    fetch_row(0)
    chunk_copy(0).start()
    chunk_copy(1).start()
    entry_barrier(peers, range(1, PARTS))
    for c in every:
        c.start()
    dw_acc[...] = jnp.zeros_like(dw_acc)

    def step(i, carry):
        stage_of(i, 1, rows, last_sends)
        stage_of(i + 4, EARLY, rows - EARLY, lambda b: half_sends(b + EARLY))
        stage_of(i, 0, rows, fetch_half)
        stage_of(i, rows, 1, share_parts)
        stage_of(i, 3, rows, fetch_last)
        stage_of(i + 1, 1, rows - 1, lambda b: fetch_row(b + 1))
        stage_of(i, 0, rows, weight_grad)
        stage_of(i, 0, rows, half_sum)
        stage_of(i, 1, chunks, project_out)
        stage_of(i, rows + 1, 1, merge_parts)
        stage_of(i, rows + 2, 1, share_mods)
        stage_of(i, 3, rows, last_sum)
        return carry

    lax.fori_loop(0, rows + 3, step, 0)
    share_parts(1)
    tile = dw_out.shape[0] // 3
    copies = [pltpu.make_async_copy(y_slot.at[n % 2, pl.ds(0, tile), :], dw_out.at[pl.ds(n * tile, tile), :], dw_sem.at[n]) for n in range(3)]
    for n, c in enumerate(copies):
        if n == 2:
            copies[0].wait()
        y_slot[n % 2, pl.ds(0, tile), :] = dw_acc[pl.ds(n * tile, tile), :].astype(BF16)
        c.start()
    merge_parts(1)
    share_mods(1)
    for c in copies[1:]:
        c.wait()
    for b in range(rows - ring, rows):
        wait_bytes(last_in.at[b], last_send.at[b])
    for n in range(2):
        dx_copy(rows - 1 - n).wait()
        xo_copy(chunks - 1 - n).wait()
    for b in range(EARLY, rows):
        wait_bytes(half_in.at[b], half_send.at[b])
    for g in range(2):
        some = mod_in.at[g, pl.ds(0, PARTS - 1)]
        wait_bytes(some, part_send.at[g])
        wait_bytes(some, mod_send.at[g])
        wait_bytes(some, mod_recv.at[g])


def scatter_grads(pairs, halves, dqkv, y_rows, o_rows, wo_full, x_loc, d_out, scale_rows, gate_rows, b_o):
    rows, seq, dim = y_rows.shape
    all_cols = dqkv.shape[2]
    seg = seq // PARTS
    group = rows // 2
    width = 256
    hbm = pl.BlockSpec(memory_space=pl.ANY)
    vmem = pl.BlockSpec(memory_space=pltpu.VMEM)
    dma = pltpu.SemaphoreType.DMA
    two, each = dma((2,)), dma((rows,))
    local = jax.ShapeDtypeStruct((rows, seg, dim), BF16)
    shard = pltpu.VMEM((rows, seg, dim), BF16)
    return pl.pallas_call(
        scatter_kernel,
        out_shape=(local, local, jax.ShapeDtypeStruct((2, 3, group, dim), F32), jax.ShapeDtypeStruct((all_cols, dim), BF16),
                   jax.ShapeDtypeStruct((rows, 2, seg // 2, dim), BF16), jax.ShapeDtypeStruct((rows, 2, seg, dim), BF16)),
        in_specs=[hbm] * 8 + [vmem] * 3,
        out_specs=[hbm] * 2 + [vmem] + [hbm] * 3,
        scratch_shapes=[pltpu.VMEM((2, seq, all_cols), BF16), pltpu.VMEM((2, seq, dim), BF16), pltpu.VMEM((all_cols, seq), BF16),
                        pltpu.VMEM((4, 2, seg, dim), BF16), pltpu.VMEM((2, 2, seg // 2, dim), BF16),
                        pltpu.VMEM((3, seg, dim), BF16), pltpu.VMEM((all_cols, dim), F32),
                        shard, shard, shard, pltpu.VMEM((2, dim, width), BF16), pltpu.VMEM((rows, seg, width), F32),
                        pltpu.VMEM((2, rows, seg, width), BF16), pltpu.VMEM((2, seg, dim), BF16), pltpu.VMEM((2, 16, dim), F32),
                        pltpu.VMEM((2, 3, group, dim), F32), pltpu.VMEM((2, PARTS, 3, group, dim // PARTS), F32)]
        + [two, two] + [each] * 6 + [dma((2, 2)), two, dma((3,)), dma((3,))] + [two] * 7,
        compiler_params=pltpu.CompilerParams(collective_id=1, has_side_effects=True, vmem_limit_bytes=VMEM_ALL),
        name='grad_scatter',
    )(pairs, halves, dqkv, y_rows, o_rows, wo_full, x_loc, d_out, scale_rows, gate_rows, b_o)


def solution(mesh):
    def device_step(x_loc, e_loc, m_block, w_q, b_q, w_k, b_k, w_v, b_v, w_o, b_o, g_q, g_k, pos_part, dy_loc):
        model_dim = x_loc.shape[-1]
        cols = w_q.shape[1]

        mod_rows = m_block[None] + e_loc
        shift_row = mod_rows[:, 0][:, None]
        scale_one = 1.0 + mod_rows[:, 1][:, None]
        gate_row = mod_rows[:, 2][:, None]
        x_float = x_loc.astype(jnp.float32)
        centered = x_float - jnp.mean(x_float, axis=-1, keepdims=True)
        inv_std = lax.rsqrt(jnp.mean(centered * centered, axis=-1, keepdims=True) + EPS_NORM)
        x_norm = centered * inv_std
        y_loc = (x_norm * scale_one + shift_row).astype(jnp.bfloat16)
        dy_float = dy_loc.astype(jnp.float32)
        dp_loc = (dy_float * gate_row).astype(jnp.bfloat16)
        y_rows, _, dqkv, o_rows, wo_full, d_wo, _, pairs, halves, d_gains = attend_grad(
            y_loc, dp_loc, w_q, w_k, w_v, jnp.concatenate([b_q, b_k, b_v])[None], jnp.concatenate([g_q, g_k])[None], rope_tables(pos_part), w_o)
        d_gq, d_gk = d_gains[0, :cols], d_gains[0, cols:]
        x_out, d_x, d_mods, dw_turned = scatter_grads(pairs, halves, dqkv, y_rows, o_rows, wo_full, x_loc, dy_loc,
                                                      scale_one[:, 0], gate_row[:, 0], b_o[None])[:4]
        d_wq, d_wk, d_wv = (dw_turned[n * cols:(n + 1) * cols].T for n in range(3))
        d_mod = jnp.moveaxis(d_mods, 1, 2).reshape(e_loc.shape)
        return (x_out, d_x, d_mod, jnp.sum(d_mod, axis=0), d_wq, d_wk, d_wv, d_wo, d_gq, d_gk)

    in_specs = (P('dp', 'tp', None), P('dp', None, None), P(None, None), P(None, 'tp'), P('tp'), P(None, 'tp'), P('tp'),
                P(None, 'tp'), P('tp'), P('tp', None), P(None), P('tp'), P('tp'), P('dp', None), P('dp', 'tp', None))
    out_specs = (P('dp', 'tp', None), P('dp', 'tp', None), P('dp', None, None), P('dp', None), P('dp', 'tp'), P('dp', 'tp'),
                 P('dp', 'tp'), P(('dp', 'tp'), None), P(('dp', 'tp')), P(('dp', 'tp')))
    return jax.shard_map(device_step, mesh=mesh, in_specs=in_specs, out_specs=out_specs, check_vma=False)
```

```python
import functools

import jax
import jax.numpy as jnp
from jax import lax
from jax.experimental import pallas as pl
from jax.experimental.pallas import tpu as pltpu
from jax.sharding import PartitionSpec as P

HEAD_DIM = 128
EPS_NORM = 1e-6
ROPE_BASE = 10000.0
ROW_CONTRACT = (((0,), (0,)), ((), ()))
COL_CONTRACT = (((1,), (1,)), ((), ()))
MESH = pl.DeviceIdType.MESH
F32 = jnp.float32
BF16 = jnp.bfloat16
PARTS = 8
PANEL = 1024
EARLY = 14
FEW = 16
VMEM_ALL = 67043328
SCORE_SCALE = HEAD_DIM ** -0.5 * 1.4426950408889634


def rope_angles(positions):
    half_dim = HEAD_DIM // 2
    side_len = HEAD_DIM // 6
    first_len = half_dim - 2 * side_len
    pair_idx = jnp.arange(half_dim)
    section = (pair_idx >= first_len).astype(jnp.int32) + (pair_idx >= first_len + side_len).astype(jnp.int32)
    offset = jnp.where(section == 0, 0, jnp.where(section == 1, first_len, first_len + side_len))
    sec_width = jnp.where(section == 0, first_len, side_len)
    freq_vals = ROPE_BASE ** (-(pair_idx - offset).astype(jnp.float32) / sec_width.astype(jnp.float32))
    select = jnp.where(section[None, :] == jnp.arange(3)[:, None], freq_vals[None, :], 0.0)
    angles = jnp.sum(positions.astype(jnp.float32)[:, :, None] * select[None, :, :], axis=1)
    return jnp.cos(angles), jnp.sin(angles)


def fill_tables(tabs, cos_tab, sin_tab):
    odd = lax.rem(lax.broadcasted_iota(jnp.int32, (1, HEAD_DIM), 1), 2).astype(F32)
    cos, sin = cos_tab[...].T, sin_tab[...].T
    up = sin * (odd - 1.0)
    down = sin * odd
    for n, (tab, scale) in enumerate(((cos, 1.0), (up, -1.0), (down, -1.0))):
        tabs[n] = tab
        tabs[n + 3] = tab * (scale * HEAD_DIM ** -0.5)


def fill_mods(mods, e_rows, m_rows):
    for n in range(3):
        mods[n] = e_rows[n] + m_rows[n:n + 1, :] + float(n == 1)


class Peers:
    def __init__(self):
        me = lax.axis_index('tp')
        self.me = me
        core, col, row = lax.rem(me, 2), lax.rem(me // 2, 2), me // 4

        def flip(bits):
            out = me
            if bits & 1:
                out = out + 1 - 2 * core
            if bits & 2:
                out = out + 2 - 4 * col
            if bits & 4:
                out = out + 4 - 8 * row
            return out

        self.at = [flip(bits) for bits in range(PARTS)]
        self.partner, self.x, self.y, self.diag = (self.at[bits] for bits in (1, 2, 4, 6))


def entry_barrier(peers, which):
    barrier = pltpu.get_barrier_semaphore()
    for bits in which:
        pl.semaphore_signal(barrier, inc=1, device_id={'tp': peers.at[bits]}, device_id_type=MESH)
    pl.semaphore_wait(barrier, len(which))


def wait_local(ref, sem):
    pltpu.make_async_copy(ref, ref, sem).wait()


def wait_bytes(ref, sem):
    pltpu.make_async_copy(ref, ref, sem).wait()


def even(b):
    return lax.rem(b, 2)


class RowGather:
    def __init__(self, peers, src, full, sems, seg):
        self.peers, self.src, self.full, self.seg = peers, src, full, seg
        self.send_sem, self.rx, self.ry, self.rd0, self.rd1, self.rp = sems
        self.lower, self.upper = (0, seg // 2), (seg // 2, seg // 2)

    def piece(self, b, t, part=None):
        lo, n = part or (0, self.seg)
        return self.full.at[b, pl.ds(pl.multiple_of(t * self.seg + lo, 32), n), :]

    def first(self, b, pieces):
        return self.full.at[b, pl.ds(0, pieces * self.seg), :]

    def send(self, src, dst, b, sem, t):
        pltpu.make_async_remote_copy(src_ref=src, dst_ref=dst, send_sem=self.send_sem.at[b], recv_sem=sem.at[b],
                                     device_id={'tp': t}, device_id_type=MESH).start()

    def own(self, b):
        p = self.peers
        for sem, t in ((self.rx, p.x), (self.ry, p.y), (self.rp, p.partner)):
            self.send(self.src(b), self.piece(b, p.me), b, sem, t)

    def direct(self, b):
        p = self.peers
        for near, sem, part, diag_sem, far in ((p.x, self.rx, self.lower, self.rd0, p.y), (p.y, self.ry, self.upper, self.rd1, p.x)):
            whole, some = self.piece(b, near), self.piece(b, near, part)
            wait_bytes(whole, sem.at[b])
            self.send(some, some, b, diag_sem, far)
            self.send(whole, whole, b, self.rp, p.partner)

    def diagonal(self, b):
        p = self.peers
        wait_bytes(self.piece(b, p.diag, self.lower), self.rd0.at[b])
        wait_bytes(self.piece(b, p.diag, self.upper), self.rd1.at[b])
        self.send(self.piece(b, p.diag), self.piece(b, p.diag), b, self.rp, p.partner)

    def complete(self, b):
        wait_bytes(self.first(b, 4), self.rp.at[b])

    def load(self, b, slot, sem):
        for n, t in enumerate(self.peers.at):
            src = self.piece(b, t) if n else self.src(b)
            pltpu.make_async_copy(src, slot.at[pl.ds(pl.multiple_of(t * self.seg, self.seg), self.seg), :], sem).start()

    def drain(self, b):
        wait_bytes(self.first(b, PARTS - 1), self.send_sem.at[b])


def stage_of(i, lag, count, work):
    @pl.when((i >= lag) & (i < count + lag))
    def _():
        work(i - lag)


def ahead_of(i, lead, count, work):
    stage_of(i + lead, lead, count - lead, lambda b: work(b + lead))


def attend_kernel(x_loc, d_out, wq, wk, wv, bq, bk, bv, gq, gk, cos_tab, sin_tab, wo, e_rows, m_rows,
                  y_own, d_own, y_full, dp_full, dqkv_out, o_tok, wo_full, dwo_out, pair_in, pair_out, half_out, dg_out,
                  w_all, y_slot, d_slot, qk_ring, v_ring, rot, o_stage, datt, dqk, dqs, dqkv_stage, col_inv, p_buf, ds_buf,
                  dwo_acc, stage, pair_stage, pair_buf, norm_buf, stat_buf,
                  y_sems, d_sems, wo_sems, w_sem, y_sem, d_sem, keep_sem, norm_send, norm_recv, stat_send, stat_recv,
                  o_send, o_keep, o_recv, out_sem, pair_send, pair_recv, pair_load, pair_sem, wo_keep, z_send, z_recv, dwo_sem, half_send, half_recv,
                  raw, own_stage, raw_sem, own_sem, bias, gains, tabs, mods):
    peers = Peers()
    me = peers.me
    depth = lax.axis_index('dp')
    sums = (norm_buf, norm_send, norm_recv), (stat_buf, stat_send, stat_recv)
    rows, seg, dim = x_loc.shape
    seq = seg * PARTS
    cols = wq.shape[1]
    heads = cols // HEAD_DIM
    blk = HEAD_DIM
    blocks = seq // blk
    wide = 2 * cols
    hemi = dim // 2
    weights = [pltpu.make_async_copy(w, w_all.at[:, pl.ds(n * cols, cols)], w_sem.at[n]) for n, w in enumerate((wq, wk, wv))]

    def raw_copy(kind, b):
        return pltpu.make_async_copy((x_loc, d_out)[kind].at[b], raw.at[kind, even(b)], raw_sem.at[kind, even(b)])

    def own_copy(kind, b):
        return pltpu.make_async_copy(own_stage.at[kind, even(b)], (y_own, d_own)[kind].at[b], own_sem.at[kind, even(b)])

    for b in range(2):
        raw_copy(0, b).start()
        raw_copy(1, b).start()
    for c in weights:
        c.start()
    fill_mods(mods, e_rows, m_rows)
    barrier = pltpu.get_barrier_semaphore()
    for t in peers.at[1:]:
        pl.semaphore_signal(barrier, inc=1, device_id={'tp': t}, device_id_type=MESH)
    pl.semaphore_signal(barrier, inc=1, device_id={'dp': 1 - depth}, device_id_type=MESH)
    pl.semaphore_wait(barrier, PARTS)
    gy = RowGather(peers, lambda b: y_own.at[b], y_full, y_sems, seg)
    gd = RowGather(peers, lambda b: d_own.at[b], dp_full, d_sems, seg)
    gw = RowGather(peers, lambda b: wo.at[:, pl.ds(pl.multiple_of(b * hemi, HEAD_DIM), hemi)], wo_full, wo_sems, cols)

    def prepare(kind):
        def work(b):
            raw_copy(kind, b).wait()
            s = even(b)
            shift, scale, gate = (mods[n, pl.ds(b, 1), :] for n in range(3))
            for n in range(seg // FEW):
                sl = pl.ds(n * FEW, FEW)
                x = raw[kind, s, sl, :].astype(F32)
                if kind == 0:
                    x = x - jnp.mean(x, axis=-1, keepdims=True)
                    x = x * lax.rsqrt(jnp.mean(x * x, axis=-1, keepdims=True) + EPS_NORM)
                    x = x * scale + shift
                else:
                    x = x * gate
                own_stage[kind, s, sl, :] = x.astype(BF16)
            own_copy(kind, b).start()

            @pl.when(b + 2 < rows)
            def _():
                raw_copy(kind, b + 2).start()
        return work

    def own_row(kind):
        def work(b):
            own_copy(kind, b).wait()
            (gy, gd)[kind].own(b)
        return work

    for kind, b in ((0, 0), (1, 0), (0, 1)):
        prepare(kind)(b)
        own_row(kind)(b)
    prepare(1)(1)
    fill_tables(tabs, cos_tab, sin_tab)
    for n, part in enumerate((bq, bk, bv)):
        bias[0, pl.ds(n * cols, cols)] = part[...]
    for n, part in enumerate((gq, gk)):
        gains[0, pl.ds(n * cols, cols)] = part[...]
    dwo_acc[...] = jnp.zeros_like(dwo_acc)
    dg_out[...] = jnp.zeros_like(dg_out)
    for c in weights:
        c.wait()

    def mine(b, width):
        return pl.ds(pl.multiple_of(b * width, width), width)

    keep_y = pltpu.make_async_copy(y_slot.at[mine(me, seg), :], gy.piece(0, me), keep_sem)

    def out_copy(b):
        return pltpu.make_async_copy(dqkv_stage.at[even(b)], dqkv_out.at[b], out_sem.at[even(b)])

    def pair_copy(b):
        return pltpu.make_async_copy(pair_stage.at[even(b)], pair_out.at[b], pair_sem.at[even(b)])

    def o_rows(b, t):
        return o_stage.at[even(b), mine(t, seg), :]

    def keep_o(b):
        return pltpu.make_async_copy(o_rows(b, me), o_tok.at[b, :, mine(me, cols)], o_keep.at[even(b)])

    def keep_wo(h):
        return pltpu.make_async_copy(gw.src(h), wo_full.at[h, mine(me, cols), :], wo_keep.at[h])

    def remote(src, dst, send, recv, device):
        return pltpu.make_async_remote_copy(src_ref=src, dst_ref=dst, send_sem=send, recv_sem=recv, device_id=device, device_id_type=MESH)

    def share(n):
        buf, send, recv = sums[n]

        def work(b):
            for t in peers.at[1:]:
                remote(buf.at[me, b], buf.at[me, b], send, recv.at[b], {'tp': t}).start()
        return work

    def sum_of(n, b):
        return jnp.sum(sums[n][0][:, b], axis=0) * (1.0 / dim)

    def send_row(b):
        share(1)(b)
        for t in peers.at[1:]:
            remote(o_rows(b, t), o_tok.at[b, :, mine(me, cols)], o_send.at[even(b)], o_recv, {'tp': t}).start()
        keep_o(b).start()

    def wait_row_sent(b):
        wait_bytes(o_stage.at[even(b), pl.ds(0, seq - seg), :], o_send.at[even(b)])
        keep_o(b).wait()

    def pair_sends(b):
        for n in range(4):
            t = peers.at[1 ^ (2 * n)]
            remote(stage.at[mine(t, seg), :], pair_in.at[b, n], pair_send, pair_recv.at[b], {'tp': peers.at[1]}).start()

    def spread(row):
        return jnp.broadcast_to(row, (blk, blk)).T

    def turned(x, sl, kind):
        c, up, down = tabs[kind, sl, :], tabs[kind + 1, sl, :], tabs[kind + 2, sl, :]
        return x * c + pltpu.roll(x, HEAD_DIM - 1, 1) * up + pltpu.roll(x, 1, 1) * down

    def lane_cols(part, h):
        return pl.ds(part * cols + h * HEAD_DIM, HEAD_DIM)

    def load_y(b):
        gy.complete(b)

        @pl.when(b >= 1)
        def _():
            keep_y.wait()

        gy.load(b, y_slot, y_sem)

    def load_d(b):
        gd.complete(b)
        gd.load(b, d_slot.at[even(b)], d_sem.at[even(b)])

    def qkv(b):
        ring = lax.rem(b, 4)
        wait_local(y_slot, y_sem)
        pltpu.make_async_copy(y_slot.at[mine(me, seg), :], gy.piece(b, me), keep_sem).start()
        tile = 2 * blk
        for m in range(seq // tile):
            sl = pl.ds(m * tile, tile)
            acc = jnp.dot(y_slot[sl, :], w_all[...], preferred_element_type=F32) + bias[...]
            qk_ring[ring, sl, :] = acc[:, :wide]
            v_ring[even(b), sl, :] = acc[:, wide:].astype(BF16)
        for j in range(blocks):
            for part in range(2):
                total = None
                for h in range(heads):
                    x = qk_ring[ring, pl.ds(j * blk, blk), lane_cols(part, h)]
                    total = x * x if total is None else total + x * x
                norm_buf[me, b, pl.ds(part * blocks + j, 1), :] = jnp.sum(total.T, axis=0, keepdims=True)

    def inv_norms(b):
        return lax.rsqrt(sum_of(0, b) + EPS_NORM)

    def attend(b):
        s, ring = even(b), lax.rem(b, 4)
        wait_bytes(norm_buf.at[pl.ds(0, PARTS - 1), b], norm_recv.at[b])
        wait_local(d_slot.at[s], d_sem.at[s])

        @pl.when(b >= 2)
        def _():
            wait_row_sent(b - 2)
            out_copy(b - 2).wait()

        tile = 2 * blk
        for m in range(seq // tile):
            sl = pl.ds(m * tile, tile)
            datt[sl, :] = lax.dot_general(d_slot[s, sl, :], wo[...], COL_CONTRACT, preferred_element_type=F32).astype(BF16)

        inv = inv_norms(b)
        for j in range(blocks):
            sl = pl.ds(j * blk, blk)
            for part in range(2):
                row = part * blocks + j
                scale = spread(inv[row:row + 1, :])
                col_inv[s, part, sl, :] = scale
                for h in range(heads):
                    cs = lane_cols(part, h)
                    rot[sl, cs] = turned(qk_ring[ring, sl, cs] * scale * gains[:, cs], sl, 0).astype(BF16)

        def head(h, carry):
            hq, hk, hv = (pl.ds(pl.multiple_of(n * cols + h * HEAD_DIM, HEAD_DIM), HEAD_DIM) for n in range(3))
            k_h, v_h = rot[:, hk], v_ring[s, :, hq]
            for j in range(blocks):
                sl = pl.ds(j * blk, blk)
                sc = lax.dot_general(rot[sl, hq], k_h, COL_CONTRACT, preferred_element_type=F32) * SCORE_SCALE
                p = jnp.exp2(sc - jnp.max(sc, axis=-1, keepdims=True))
                p = p * (1.0 / jnp.sum(p, axis=-1, keepdims=True))
                pb = p.astype(BF16)
                p_buf[sl, :] = pb
                o_stage[s, sl, hq] = jnp.dot(pb, v_h, preferred_element_type=F32).astype(BF16)
                dp = lax.dot_general(datt[sl, hq], v_h, COL_CONTRACT, preferred_element_type=F32)
                ds = (p * (dp - jnp.sum(p * dp, axis=-1, keepdims=True))).astype(BF16)
                ds_buf[sl, :] = ds
                dqk[sl, hq] = jnp.dot(ds, k_h, preferred_element_type=F32)
            dqk[:, hk] = lax.dot_general(ds_buf[...], rot[:, hq], ROW_CONTRACT, preferred_element_type=F32)
            dqkv_stage[s, :, hv] = lax.dot_general(p_buf[...], datt[:, hq], ROW_CONTRACT, preferred_element_type=F32).astype(BF16)
            return carry

        lax.fori_loop(0, heads, head, 0)

        for j in range(blocks):
            sl = pl.ds(j * blk, blk)
            for part in range(2):
                scale = col_inv[s, part, sl, :]
                total = None
                for h in range(heads):
                    cs = lane_cols(part, h)
                    dx = turned(dqk[sl, cs], sl, 3)
                    prod = dx * (qk_ring[ring, sl, cs] * scale)
                    dg_out[:, cs] = dg_out[:, cs] + jnp.sum(prod, axis=0, keepdims=True)
                    dqs[s, sl, cs] = dx * gains[:, cs]
                    prod = prod * gains[:, cs]
                    total = prod if total is None else total + prod
                stat_buf[me, b, pl.ds(part * blocks + j, 1), :] = jnp.sum(total.T, axis=0, keepdims=True)

        for n in range(3):
            cs = pl.ds(n * PANEL, PANEL)
            dwo_acc[:, cs] += lax.dot_general(o_stage[s], d_slot[s, :, cs], ROW_CONTRACT, preferred_element_type=F32)

    def finish(b):
        s, ring = even(b), lax.rem(b, 4)
        wait_bytes(stat_buf.at[pl.ds(0, PARTS - 1), b], stat_recv.at[b])
        inv = inv_norms(b)
        coef = sum_of(1, b) * inv * inv
        for j in range(blocks):
            sl = pl.ds(j * blk, blk)
            for part in range(2):
                row = part * blocks + j
                scale = col_inv[s, part, sl, :]
                pull = spread(coef[row:row + 1, :])
                for h in range(heads):
                    cs = lane_cols(part, h)
                    dqkv_stage[s, sl, cs] = (scale * dqs[s, sl, cs] - pull * qk_ring[ring, sl, cs]).astype(BF16)
        out_copy(b).start()
        for n in range(3):
            cs = pl.ds(n * PANEL, PANEL)
            stage[:, cs] = lax.dot_general(dqkv_stage[s], w_all[cs, :], COL_CONTRACT, preferred_element_type=F32).astype(BF16)

    def pair_sum(b):
        wait_bytes(pair_in.at[b], pair_recv.at[b])
        load = pltpu.make_async_copy(pair_in.at[b], pair_buf, pair_load)
        load.start()

        @pl.when(b >= 1)
        def _():
            pair_copy(b - 1).wait()

        wait_bytes(pair_in.at[b], pair_send)
        load.wait()
        for n in range(4):
            pair_stage[even(b), n] = (stage[mine(peers.at[2 * n], seg), :].astype(F32) + pair_buf[n].astype(F32)).astype(BF16)
        pair_copy(b).start()

    def spread_wo(h):
        gw.complete(h)
        for t in peers.at[1:]:
            piece = gw.piece(h, t)
            remote(piece, piece, z_send, z_recv, {'dp': 1 - depth}).start()

    def half_sends(b):
        for n, t in enumerate((peers.y, peers.x)):
            remote(pair_out.at[b, 3, mine(n, seg // 2), :], half_out.at[b, n], half_send.at[b], half_recv.at[n, b], {'tp': t}).start()

    def early_halves(lo, hi):
        def work(b):
            for n in range(lo, hi):
                half_sends(n)
        return work

    def step(i, carry):
        stage_of(i, 4, rows, send_row)
        stage_of(i, rows, 1, early_halves(0, 3))
        stage_of(i, rows + 1, 1, early_halves(6, 9))
        stage_of(i, rows + 2, 1, early_halves(9, 11))
        stage_of(i, rows + 3, 1, early_halves(11, 12))
        stage_of(i, rows + 4, 1, early_halves(12, 13))
        stage_of(i, rows + 5, 1, early_halves(13, EARLY))
        ahead_of(i, 2, rows, prepare(0))
        ahead_of(i, 1, rows, own_row(1))
        stage_of(i, 0, rows, gy.direct)
        stage_of(i, 1, rows, gy.diagonal)
        stage_of(i, 2, rows, load_d)
        stage_of(i, 2, 1, lambda b: gw.own(depth))
        stage_of(i, 4, 1, lambda b: gw.direct(depth))
        stage_of(i, 5, 1, lambda b: gw.diagonal(depth))
        stage_of(i, 6, 1, lambda b: spread_wo(depth))
        stage_of(i, 2, rows, qkv)
        stage_of(i, 6, rows, pair_sum)
        stage_of(i, 5, rows, finish)
        stage_of(i, 2, rows, share(0))
        stage_of(i, 5, rows, pair_sends)
        stage_of(i, rows, 1, early_halves(3, 6))
        ahead_of(i, 2, rows, prepare(1))
        ahead_of(i, 2, rows, own_row(0))
        stage_of(i, 0, rows, gd.direct)
        stage_of(i, 1, rows, gd.diagonal)
        stage_of(i, 1, rows, load_y)
        stage_of(i, 3, rows, attend)
        return carry

    keep_wo(0).start()
    keep_wo(1).start()
    lax.fori_loop(0, rows + 6, step, 0)
    stage[pl.ds(0, cols), :] = dwo_acc[...].astype(BF16)
    dwo_copy = pltpu.make_async_copy(stage.at[pl.ds(0, cols), :], dwo_out, dwo_sem)
    dwo_copy.start()
    keep_y.wait()
    keep_wo(0).wait()
    keep_wo(1).wait()
    for b in (rows - 2, rows - 1):
        wait_row_sent(b)
        out_copy(b).wait()
    pair_copy(rows - 1).wait()

    def drain(b, carry):
        gy.drain(b)
        gd.drain(b)
        return carry

    lax.fori_loop(0, rows, drain, 0)
    gw.drain(depth)
    for buf, send, _ in sums:
        wait_bytes(buf.at[pl.ds(0, PARTS - 1)], send)
    wait_bytes(o_tok.at[pl.ds(0, rows - rows // PARTS)], o_recv)
    sent = wo_full.at[0, pl.ds(0, dim - cols), :]
    wait_bytes(sent, z_send)
    wait_bytes(sent, z_recv)
    dwo_copy.wait()
    for b in range(EARLY):
        wait_bytes(half_out.at[b], half_send.at[b])
        for n in range(2):
            wait_bytes(half_out.at[b, n], half_recv.at[n, b])


def attend_grad(x_loc, d_out, w_q, w_k, w_v, small, w_o, mod_parts):
    rows, seg, dim = x_loc.shape
    cols = w_o.shape[0]
    seq = seg * PARTS
    hbm = pl.BlockSpec(memory_space=pl.ANY)
    vmem = pl.BlockSpec(memory_space=pltpu.VMEM)
    dma = pltpu.SemaphoreType.DMA
    two, each = dma((2,)), dma((rows,))
    gathered = jax.ShapeDtypeStruct((rows, seq, dim), BF16)
    paired = jax.ShapeDtypeStruct((rows, 4, seg, dim), BF16)
    local = jax.ShapeDtypeStruct((rows, seg, dim), BF16)
    local_ring = pltpu.VMEM((2, 2, seg, dim), BF16)
    wide, all_cols = 2 * cols, 3 * cols
    partials = pltpu.VMEM((PARTS, rows, 8, HEAD_DIM), F32)
    return pl.pallas_call(
        attend_kernel,
        out_shape=(local, local, gathered, gathered, jax.ShapeDtypeStruct((rows, seq, all_cols), BF16), jax.ShapeDtypeStruct((rows, seg, dim), BF16),
                   jax.ShapeDtypeStruct((2, dim, dim // 2), BF16), jax.ShapeDtypeStruct((cols, dim), BF16), paired, paired,
                   jax.ShapeDtypeStruct((EARLY, 2, seg // 2, dim), BF16),
                   jax.ShapeDtypeStruct((1, wide), F32)),
        in_specs=[hbm] * 5 + [vmem] * 10,
        out_specs=[hbm] * 11 + [vmem],
        scratch_shapes=[pltpu.VMEM((dim, all_cols), BF16), pltpu.VMEM((seq, dim), BF16), pltpu.VMEM((2, seq, dim), BF16),
                        pltpu.VMEM((4, seq, wide), F32), pltpu.VMEM((2, seq, cols), BF16), pltpu.VMEM((seq, wide), BF16),
                        pltpu.VMEM((2, seq, cols), BF16), pltpu.VMEM((seq, cols), BF16), pltpu.VMEM((seq, wide), F32),
                        pltpu.VMEM((2, seq, wide), F32), pltpu.VMEM((2, seq, all_cols), BF16), pltpu.VMEM((2, 2, seq, HEAD_DIM), F32),
                        pltpu.VMEM((seq, seq), BF16), pltpu.VMEM((seq, seq), BF16), pltpu.VMEM((cols, dim), F32), pltpu.VMEM((seq, dim), BF16),
                        pltpu.VMEM((2, 4, seg, dim), BF16), pltpu.VMEM((4, seg, dim), BF16),
                        partials, partials]
        + [[each] * 6, [each] * 6, [two] * 6, dma((3,)), dma, two, dma, dma, each, dma, each,
           two, two, dma, two, dma, each, dma, two, two, dma, dma, dma, dma((EARLY,)), dma((2, EARLY)),
           local_ring, local_ring, dma((2, 2)), dma((2, 2)),
           pltpu.VMEM((1, all_cols), F32), pltpu.VMEM((1, wide), F32), pltpu.VMEM((6, seq, HEAD_DIM), F32), pltpu.VMEM((3, rows, dim), F32)],
        compiler_params=pltpu.CompilerParams(collective_id=0, has_side_effects=True, vmem_limit_bytes=VMEM_ALL),
        name='gather_attend',
    )(x_loc, d_out, w_q, w_k, w_v, *small, w_o, *mod_parts)


def scatter_kernel(pairs, halves, dqkv, y_full, o_tok, wo_full, x_loc, d_out, e_rows, m_rows, b_o,
                   xo_out, dx_out, mod_out, dwq_out, dwk_out, dwv_out, half_in, last_in,
                   dt_slot, y_slot, half_stage, half_buf, last_buf, dw_acc,
                   o_all, x_all, dy_all, w_slot, proj, xo_stage, dx_stage, sums, mod_part, mod_in,
                   dt_sem, y_sem, half_send, last_send, half_recv0, half_recv1, last_recv0, last_recv1, half_load, last_load, dw_sem,
                   all_sem, wch_sem, xo_sem, dx_sem, part_send, part_recv, mod_send, mod_recv, mods):
    peers = Peers()
    me = peers.me
    rows, seq, dim = y_full.shape
    seg = seq // PARTS
    half = seg // 2
    cols = dim // PARTS
    width = w_slot.shape[2]
    chunks = dim // width
    group = mod_part.shape[2]
    every = [pltpu.make_async_copy(src, dst, all_sem.at[n]) for n, (src, dst) in enumerate(((o_tok, o_all), (x_loc, x_all), (d_out, dy_all)))]

    def mine(b, size):
        return pl.ds(pl.multiple_of(b * size, size), size)

    def dt_copy(b):
        return pltpu.make_async_copy(dqkv.at[b], dt_slot.at[even(b)], dt_sem.at[even(b)])

    def y_copy(b):
        return pltpu.make_async_copy(y_full.at[b], y_slot.at[even(b)], y_sem.at[even(b)])

    def dx_copy(b):
        return pltpu.make_async_copy(dx_stage.at[even(b)], dx_out.at[b], dx_sem.at[even(b)])

    def chunk_copy(n):
        per = chunks // 2
        return pltpu.make_async_copy(wo_full.at[n // per, :, mine(lax.rem(n, per), width)], w_slot.at[even(n)], wch_sem.at[even(n)])

    def xo_copy(n):
        return pltpu.make_async_copy(xo_stage.at[even(n)], xo_out.at[:, :, mine(n, width)], xo_sem.at[even(n)])

    def remote(src, dst, send, recv, t):
        pltpu.make_async_remote_copy(src_ref=src, dst_ref=dst, send_sem=send, recv_sem=recv,
                                     device_id={'tp': t}, device_id_type=MESH).start()

    def half_sends(b):
        remote(pairs.at[b, 3, pl.ds(0, half), :], half_in.at[b, 0], half_send.at[b], half_recv0.at[b], peers.y)
        remote(pairs.at[b, 3, pl.ds(half, half), :], half_in.at[b, 1], half_send.at[b], half_recv1.at[b], peers.x)

    ring = half_stage.shape[0]

    def last_sends(b):
        s = lax.rem(b, ring)
        remote(half_stage.at[s, 0], last_in.at[b, 0], last_send.at[b], last_recv0.at[b], peers.x)
        remote(half_stage.at[s, 1], last_in.at[b, 1], last_send.at[b], last_recv1.at[b], peers.y)

    def half_loads(b, source=None):
        s = even(b)
        return (pltpu.make_async_copy((half_in if source is None else source).at[b], half_buf.at[s], half_load.at[0, s]),
                pltpu.make_async_copy(pairs.at[b, pl.ds(1, 2)], half_stage.at[lax.rem(b, ring)], half_load.at[1, s]))

    def last_loads(b):
        return (pltpu.make_async_copy(last_in.at[b], last_buf.at[pl.ds(0, 2)], last_load.at[0]),
                pltpu.make_async_copy(pairs.at[b, 0], last_buf.at[2], last_load.at[1]))

    def fetch_half(b):
        @pl.when(b >= ring)
        def _():
            wait_bytes(last_in.at[b - ring], last_send.at[b - ring])

        @pl.when(b < EARLY)
        def _():
            for c in half_loads(b, halves):
                c.start()

        @pl.when(b >= EARLY)
        def _():
            wait_bytes(half_in.at[b, 0], half_recv0.at[b])
            wait_bytes(half_in.at[b, 1], half_recv1.at[b])
            for c in half_loads(b):
                c.start()

    def half_sum(b):
        s, r = even(b), lax.rem(b, ring)
        for c in half_loads(b):
            c.wait()
        for n in range(2):
            sl = pl.ds(n * half, half)
            half_stage[r, n, sl, :] = (half_stage[r, n, sl, :].astype(F32) + half_buf[s, n].astype(F32)).astype(BF16)

    def fetch_last(b):
        wait_bytes(last_in.at[b, 0], last_recv0.at[b])
        wait_bytes(last_in.at[b, 1], last_recv1.at[b])
        for c in last_loads(b):
            c.start()

    def last_sum(b):
        for c in last_loads(b):
            c.wait()

        @pl.when(b >= 2)
        def _():
            dx_copy(b - 2).wait()

        sums[...] = jnp.zeros_like(sums)
        few = FEW // 2
        scale = mods[1, pl.ds(b, 1), :]

        def tokens(n, carry):
            sl = mine(n, FEW)
            dy = last_buf[2, sl, :].astype(F32) + last_buf[0, sl, :].astype(F32) + last_buf[1, sl, :].astype(F32)
            x = x_all[b, sl, :].astype(F32)
            x = x - jnp.mean(x, axis=-1, keepdims=True)
            inv_std = lax.rsqrt(jnp.mean(x * x, axis=-1, keepdims=True) + EPS_NORM)
            x = x * inv_std
            sums[0] += dy[:few] + dy[few:]
            prod = dy * x
            sums[1] += prod[:few] + prod[few:]
            dn = dy * scale
            pull = x * jnp.mean(dn * x, axis=-1, keepdims=True) + jnp.mean(dn, axis=-1, keepdims=True)
            dx_stage[even(b), sl, :] = (dy_all[b, sl, :].astype(F32) + inv_std * (dn - pull)).astype(BF16)
            return carry

        lax.fori_loop(0, seg // FEW, tokens, 0)
        dx_copy(b).start()
        for n in range(2):
            mod_part[b // group, n, pl.ds(lax.rem(b, group), 1), :] = jnp.sum(sums[n], axis=0, keepdims=True)

    def project_out(n):
        cs = mine(n, width)

        @pl.when(n == 0)
        def _():
            for c in every:
                c.wait()

        @pl.when(n >= 2)
        def _():
            xo_copy(n - 2).wait()

        chunk_copy(n).wait()
        flat = o_all[...].reshape(rows * seg, dim)
        proj[...] = (jnp.dot(flat, w_slot[even(n)], preferred_element_type=F32) + b_o[:, cs]).reshape(proj.shape)

        def row(b, carry):
            out = proj[b]
            xo_stage[even(n), b] = (x_all[b, :, cs].astype(F32) + mods[2, pl.ds(b, 1), cs] * out).astype(BF16)
            mod_part[b // group, 2, pl.ds(lax.rem(b, group), 1), cs] = jnp.sum(dy_all[b, :, cs].astype(F32) * out, axis=0, keepdims=True)
            return carry

        lax.fori_loop(0, rows, row, 0)
        xo_copy(n).start()

        @pl.when(n + 2 < chunks)
        def _():
            chunk_copy(n + 2).start()

    def fetch_row(b):
        y_copy(b).start()
        dt_copy(b).start()

    def weight_grad(b):
        s = even(b)
        y_copy(b).wait()
        dt_copy(b).wait()
        for n in range(6):
            sl = pl.ds(n * (PANEL // 2), PANEL // 2)
            dw_acc[sl, :] += lax.dot_general(y_slot[s, :, sl], dt_slot[s], ROW_CONTRACT, preferred_element_type=F32)

    def share_parts(g):
        for t in peers.at[1:]:
            remote(mod_part.at[g, :, :, mine(t, cols)], mod_in.at[g, me], part_send.at[g], part_recv.at[g], t)
        mod_in[g, me] = mod_part[g, :, :, mine(me, cols)]

    def merge_parts(g):
        wait_bytes(mod_in.at[g, pl.ds(0, PARTS - 1)], part_recv.at[g])
        mod_out[g, :, :, mine(me, cols)] = jnp.sum(mod_in[g], axis=0)

    def share_mods(g):
        here = mod_out.at[g, :, :, mine(me, cols)]
        for t in peers.at[1:]:
            remote(here, here, mod_send.at[g], mod_recv.at[g], t)

    fetch_row(0)
    chunk_copy(0).start()
    chunk_copy(1).start()
    entry_barrier(peers, range(1, PARTS))
    for c in every:
        c.start()
    for b in range(EARLY, rows):
        half_sends(b)
    for b in range(2):
        fetch_half(b)
    fill_mods(mods, e_rows, m_rows)
    half_sum(0)
    half_sum(1)
    fetch_half(2)
    last_sends(0)
    dw_acc[...] = jnp.zeros_like(dw_acc)
    half_sum(2)
    last_sends(1)

    def step(i, carry):
        ahead_of(i, 2, rows, last_sends)
        ahead_of(i, 3, rows, fetch_half)
        stage_of(i, rows - 1, 1, share_parts)
        ahead_of(i, 1, rows, fetch_row)
        stage_of(i, 0, rows, weight_grad)
        stage_of(i, 2, rows, fetch_last)
        ahead_of(i, 3, rows, half_sum)
        stage_of(i, 1, chunks, project_out)
        stage_of(i, rows, 1, merge_parts)
        stage_of(i, rows + 1, 1, share_mods)
        stage_of(i, 2, rows, last_sum)
        return carry

    lax.fori_loop(0, rows + 2, step, 0)
    share_parts(1)
    tile = dt_slot.shape[1]
    turns = dim // tile
    own_cols = dwq_out.shape[1]
    copies = [[pltpu.make_async_copy(dt_slot.at[n % 2, :, pl.ds(k * own_cols, own_cols)], out.at[pl.ds(n * tile, tile), :], dw_sem.at[n, k])
               for k, out in enumerate((dwq_out, dwk_out, dwv_out))] for n in range(turns)]
    for n in range(turns):
        if n >= 2:
            for c in copies[n - 2]:
                c.wait()
        dt_slot[n % 2] = dw_acc[pl.ds(n * tile, tile), :].astype(BF16)
        for c in copies[n]:
            c.start()
    merge_parts(1)
    share_mods(1)
    for c in copies[turns - 2] + copies[turns - 1]:
        c.wait()
    for b in range(rows - ring, rows):
        wait_bytes(last_in.at[b], last_send.at[b])
    for n in range(2):
        dx_copy(rows - 1 - n).wait()
        xo_copy(chunks - 1 - n).wait()
    for b in range(EARLY, rows):
        wait_bytes(half_in.at[b], half_send.at[b])
    for g in range(2):
        some = mod_in.at[g, pl.ds(0, PARTS - 1)]
        wait_bytes(some, part_send.at[g])
        wait_bytes(some, mod_send.at[g])
        wait_bytes(some, mod_recv.at[g])


def scatter_grads(pairs, halves, dqkv, y_rows, o_rows, wo_full, x_loc, d_out, mod_parts, b_o):
    rows, seq, dim = y_rows.shape
    all_cols = dqkv.shape[2]
    seg = seq // PARTS
    group = rows // 2
    width = 256
    hbm = pl.BlockSpec(memory_space=pl.ANY)
    vmem = pl.BlockSpec(memory_space=pltpu.VMEM)
    dma = pltpu.SemaphoreType.DMA
    two, each = dma((2,)), dma((rows,))
    local = jax.ShapeDtypeStruct((rows, seg, dim), BF16)
    shard = pltpu.VMEM((rows, seg, dim), BF16)
    grad = jax.ShapeDtypeStruct((dim, all_cols // 3), BF16)
    return pl.pallas_call(
        scatter_kernel,
        out_shape=(local, local, jax.ShapeDtypeStruct((2, 3, group, dim), F32), grad, grad, grad,
                   jax.ShapeDtypeStruct((rows, 2, seg // 2, dim), BF16), jax.ShapeDtypeStruct((rows, 2, seg, dim), BF16)),
        in_specs=[hbm] * 8 + [vmem] * 3,
        out_specs=[hbm] * 2 + [vmem] + [hbm] * 5,
        scratch_shapes=[pltpu.VMEM((2, seq, all_cols), BF16), pltpu.VMEM((2, seq, dim), BF16),
                        pltpu.VMEM((8, 2, seg, dim), BF16), pltpu.VMEM((2, 2, seg // 2, dim), BF16),
                        pltpu.VMEM((3, seg, dim), BF16), pltpu.VMEM((dim, all_cols), F32),
                        shard, shard, shard, pltpu.VMEM((2, dim, width), BF16), pltpu.VMEM((rows, seg, width), F32),
                        pltpu.VMEM((2, rows, seg, width), BF16), pltpu.VMEM((2, seg, dim), BF16), pltpu.VMEM((2, FEW // 2, dim), F32),
                        pltpu.VMEM((2, 3, group, dim), F32), pltpu.VMEM((2, PARTS, 3, group, dim // PARTS), F32)]
        + [two, two] + [each] * 6 + [dma((2, 2)), two, dma((dim // seq, 3)), dma((3,))] + [two] * 7 + [pltpu.VMEM((3, rows, dim), F32)],
        compiler_params=pltpu.CompilerParams(collective_id=1, has_side_effects=True, vmem_limit_bytes=VMEM_ALL),
        name='grad_scatter',
    )(pairs, halves, dqkv, y_rows, o_rows, wo_full, x_loc, d_out, *mod_parts, b_o)


def solution(mesh):
    def device_step(x_loc, e_loc, m_block, w_q, b_q, w_k, b_k, w_v, b_v, w_o, b_o, g_q, g_k, pos_part, dy_loc):
        cols = w_q.shape[1]

        mod_parts = (jnp.moveaxis(e_loc, 1, 0), m_block)
        small = [b_q, b_k, b_v, g_q, g_k] + [jnp.repeat(t.T, 2, axis=0) for t in rope_angles(pos_part)]
        _, _, y_rows, _, dqkv, o_rows, wo_full, d_wo, _, pairs, halves, d_gains = attend_grad(x_loc, dy_loc, w_q, w_k, w_v, small, w_o, mod_parts)
        d_gq, d_gk = d_gains[0, :cols], d_gains[0, cols:]
        x_out, d_x, d_mods, d_wq, d_wk, d_wv = scatter_grads(pairs, halves, dqkv, y_rows, o_rows, wo_full, x_loc, dy_loc, mod_parts, b_o[None])[:6]
        d_mod = jnp.moveaxis(d_mods, 1, 2).reshape(e_loc.shape)
        return (x_out, d_x, d_mod, jnp.sum(d_mods, axis=(0, 2)), d_wq, d_wk, d_wv, d_wo, d_gq, d_gk)

    in_specs = (P('dp', 'tp', None), P('dp', None, None), P(None, None), P(None, 'tp'), P('tp'), P(None, 'tp'), P('tp'),
                P(None, 'tp'), P('tp'), P('tp', None), P(None), P('tp'), P('tp'), P('dp', None), P('dp', 'tp', None))
    out_specs = (P('dp', 'tp', None), P('dp', 'tp', None), P('dp', None, None), P('dp', None), P('dp', 'tp'), P('dp', 'tp'),
                 P('dp', 'tp'), P(('dp', 'tp'), None), P(('dp', 'tp')), P(('dp', 'tp')))
    return jax.shard_map(device_step, mesh=mesh, in_specs=in_specs, out_specs=out_specs, check_vma=False)
```

```python
import functools

import jax
import jax.numpy as jnp
from jax import lax
from jax.experimental import pallas as pl
from jax.experimental.pallas import tpu as pltpu
from jax.sharding import PartitionSpec as P

HEAD_DIM = 128
EPS_NORM = 1e-6
ROPE_BASE = 10000.0
ROW_CONTRACT = (((0,), (0,)), ((), ()))
COL_CONTRACT = (((1,), (1,)), ((), ()))
MESH = pl.DeviceIdType.MESH
F32 = jnp.float32
BF16 = jnp.bfloat16
PARTS = 8
PANEL = 1024
EARLY = 14
FEW = 16
VMEM_ALL = 67043328
SCORE_SCALE = HEAD_DIM ** -0.5 * 1.4426950408889634


def rope_angles(positions):
    half_dim = HEAD_DIM // 2
    side_len = HEAD_DIM // 6
    first_len = half_dim - 2 * side_len
    pair_idx = jnp.arange(half_dim)
    section = (pair_idx >= first_len).astype(jnp.int32) + (pair_idx >= first_len + side_len).astype(jnp.int32)
    offset = jnp.where(section == 0, 0, jnp.where(section == 1, first_len, first_len + side_len))
    sec_width = jnp.where(section == 0, first_len, side_len)
    freq_vals = ROPE_BASE ** (-(pair_idx - offset).astype(jnp.float32) / sec_width.astype(jnp.float32))
    select = jnp.where(section[None, :] == jnp.arange(3)[:, None], freq_vals[None, :], 0.0)
    angles = jnp.sum(positions.astype(jnp.float32)[:, :, None] * select[None, :, :], axis=1)
    return jnp.cos(angles), jnp.sin(angles)


def fill_tables(tabs, cos_tab, sin_tab):
    odd = lax.rem(lax.broadcasted_iota(jnp.int32, (1, HEAD_DIM), 1), 2).astype(F32)
    cos, sin = cos_tab[...].T, sin_tab[...].T
    up = sin * (odd - 1.0)
    down = sin * odd
    for n, (tab, scale) in enumerate(((cos, 1.0), (up, -1.0), (down, -1.0))):
        tabs[n] = tab
        tabs[n + 3] = tab * (scale * HEAD_DIM ** -0.5)


def fill_mods(mods, e_rows, m_rows):
    for n in range(3):
        mods[n] = e_rows[n] + m_rows[n:n + 1, :] + float(n == 1)


class Peers:
    def __init__(self):
        me = lax.axis_index('tp')
        self.me = me
        core, col, row = lax.rem(me, 2), lax.rem(me // 2, 2), me // 4

        def flip(bits):
            out = me
            if bits & 1:
                out = out + 1 - 2 * core
            if bits & 2:
                out = out + 2 - 4 * col
            if bits & 4:
                out = out + 4 - 8 * row
            return out

        self.at = [flip(bits) for bits in range(PARTS)]
        self.partner, self.x, self.y, self.diag = (self.at[bits] for bits in (1, 2, 4, 6))


def entry_barrier(peers, which):
    barrier = pltpu.get_barrier_semaphore()
    for bits in which:
        pl.semaphore_signal(barrier, inc=1, device_id={'tp': peers.at[bits]}, device_id_type=MESH)
    pl.semaphore_wait(barrier, len(which))


def wait_local(ref, sem):
    pltpu.make_async_copy(ref, ref, sem).wait()


def wait_bytes(ref, sem):
    pltpu.make_async_copy(ref, ref, sem).wait()


def even(b):
    return lax.rem(b, 2)


class RowGather:
    def __init__(self, peers, src, full, sems, seg):
        self.peers, self.src, self.full, self.seg = peers, src, full, seg
        self.send_sem, self.rx, self.ry, self.rd0, self.rd1, self.rp = sems
        self.lower, self.upper = (0, seg // 2), (seg // 2, seg // 2)

    def piece(self, b, t, part=None):
        lo, n = part or (0, self.seg)
        return self.full.at[b, pl.ds(pl.multiple_of(t * self.seg + lo, 32), n), :]

    def first(self, b, pieces):
        return self.full.at[b, pl.ds(0, pieces * self.seg), :]

    def send(self, src, dst, b, sem, t):
        pltpu.make_async_remote_copy(src_ref=src, dst_ref=dst, send_sem=self.send_sem.at[b], recv_sem=sem.at[b],
                                     device_id={'tp': t}, device_id_type=MESH).start()

    def own(self, b):
        p = self.peers
        for sem, t in ((self.rx, p.x), (self.ry, p.y), (self.rp, p.partner)):
            self.send(self.src(b), self.piece(b, p.me), b, sem, t)

    def direct(self, b):
        p = self.peers
        for near, sem, part, diag_sem, far in ((p.x, self.rx, self.lower, self.rd0, p.y), (p.y, self.ry, self.upper, self.rd1, p.x)):
            whole, some = self.piece(b, near), self.piece(b, near, part)
            wait_bytes(whole, sem.at[b])
            self.send(some, some, b, diag_sem, far)
            self.send(whole, whole, b, self.rp, p.partner)

    def diagonal(self, b):
        p = self.peers
        wait_bytes(self.piece(b, p.diag, self.lower), self.rd0.at[b])
        wait_bytes(self.piece(b, p.diag, self.upper), self.rd1.at[b])
        self.send(self.piece(b, p.diag), self.piece(b, p.diag), b, self.rp, p.partner)

    def complete(self, b):
        wait_bytes(self.first(b, 4), self.rp.at[b])

    def load(self, b, slot, sem):
        for n, t in enumerate(self.peers.at):
            src = self.piece(b, t) if n else self.src(b)
            pltpu.make_async_copy(src, slot.at[pl.ds(pl.multiple_of(t * self.seg, self.seg), self.seg), :], sem).start()

    def drain(self, b):
        wait_bytes(self.first(b, PARTS - 1), self.send_sem.at[b])


def stage_of(i, lag, count, work):
    @pl.when((i >= lag) & (i < count + lag))
    def _():
        work(i - lag)


def ahead_of(i, lead, count, work):
    stage_of(i + lead, lead, count - lead, lambda b: work(b + lead))


def attend_kernel(x_loc, d_out, wq, wk, wv, bq, bk, bv, gq, gk, cos_tab, sin_tab, wo, e_rows, m_rows,
                  y_own, d_own, y_full, dp_full, dqkv_out, o_tok, wo_full, dwo_out, pair_in, pair_out, half_out, dg_out,
                  w_all, y_slot, d_slot, qk_ring, v_ring, rot, o_stage, datt, dqk, dqs, dqkv_stage, col_inv, p_buf, ds_buf,
                  dwo_acc, stage, pair_stage, pair_buf, norm_buf, stat_buf,
                  y_sems, d_sems, wo_sems, w_sem, y_sem, d_sem, keep_sem, norm_send, norm_recv, stat_send, stat_recv,
                  o_send, o_keep, o_recv, out_sem, pair_send, pair_recv, pair_load, pair_sem, wo_keep, z_send, z_recv, dwo_sem, half_send, half_recv,
                  raw, own_stage, raw_sem, own_sem, bias, gains, tabs, mods):
    peers = Peers()
    me = peers.me
    depth = lax.axis_index('dp')
    sums = (norm_buf, norm_send, norm_recv), (stat_buf, stat_send, stat_recv)
    rows, seg, dim = x_loc.shape
    seq = seg * PARTS
    cols = wq.shape[1]
    heads = cols // HEAD_DIM
    blk = HEAD_DIM
    blocks = seq // blk
    wide = 2 * cols
    hemi = dim // 2
    weights = [pltpu.make_async_copy(w, w_all.at[:, pl.ds(n * cols, cols)], w_sem.at[n]) for n, w in enumerate((wq, wk, wv))]

    def raw_copy(kind, b):
        return pltpu.make_async_copy((x_loc, d_out)[kind].at[b], raw.at[kind, even(b)], raw_sem.at[kind, even(b)])

    def own_copy(kind, b):
        return pltpu.make_async_copy(own_stage.at[kind, even(b)], (y_own, d_own)[kind].at[b], own_sem.at[kind, even(b)])

    for b in range(2):
        raw_copy(0, b).start()
        raw_copy(1, b).start()
    for c in weights:
        c.start()
    fill_mods(mods, e_rows, m_rows)
    barrier = pltpu.get_barrier_semaphore()
    for t in peers.at[1:]:
        pl.semaphore_signal(barrier, inc=1, device_id={'tp': t}, device_id_type=MESH)
    pl.semaphore_signal(barrier, inc=1, device_id={'dp': 1 - depth}, device_id_type=MESH)
    pl.semaphore_wait(barrier, PARTS)
    gy = RowGather(peers, lambda b: y_own.at[b], y_full, y_sems, seg)
    gd = RowGather(peers, lambda b: d_own.at[b], dp_full, d_sems, seg)
    gw = RowGather(peers, lambda b: wo.at[:, pl.ds(pl.multiple_of(b * hemi, HEAD_DIM), hemi)], wo_full, wo_sems, cols)

    def prepare(kind):
        def work(b):
            raw_copy(kind, b).wait()
            s = even(b)
            shift, scale, gate = (mods[n, pl.ds(b, 1), :] for n in range(3))
            for n in range(seg // FEW):
                sl = pl.ds(n * FEW, FEW)
                x = raw[kind, s, sl, :].astype(F32)
                if kind == 0:
                    x = x - jnp.mean(x, axis=-1, keepdims=True)
                    x = x * lax.rsqrt(jnp.mean(x * x, axis=-1, keepdims=True) + EPS_NORM)
                    x = x * scale + shift
                else:
                    x = x * gate
                own_stage[kind, s, sl, :] = x.astype(BF16)
            own_copy(kind, b).start()

            @pl.when(b + 2 < rows)
            def _():
                raw_copy(kind, b + 2).start()
        return work

    def own_row(kind):
        def work(b):
            own_copy(kind, b).wait()
            (gy, gd)[kind].own(b)
        return work

    for kind, b in ((0, 0), (1, 0), (0, 1)):
        prepare(kind)(b)
        own_row(kind)(b)
    prepare(1)(1)
    fill_tables(tabs, cos_tab, sin_tab)
    for n, part in enumerate((bq, bk, bv)):
        bias[0, pl.ds(n * cols, cols)] = part[...]
    for n, part in enumerate((gq, gk)):
        gains[0, pl.ds(n * cols, cols)] = part[...]
    dwo_acc[...] = jnp.zeros_like(dwo_acc)
    dg_out[...] = jnp.zeros_like(dg_out)
    for c in weights:
        c.wait()

    def mine(b, width):
        return pl.ds(pl.multiple_of(b * width, width), width)

    keep_y = pltpu.make_async_copy(y_slot.at[mine(me, seg), :], gy.piece(0, me), keep_sem)

    def out_copy(b):
        return pltpu.make_async_copy(dqkv_stage.at[even(b)], dqkv_out.at[b], out_sem.at[even(b)])

    def pair_copy(b):
        return pltpu.make_async_copy(pair_stage.at[even(b)], pair_out.at[b], pair_sem.at[even(b)])

    def o_rows(b, t):
        return o_stage.at[even(b), mine(t, seg), :]

    def keep_o(b):
        return pltpu.make_async_copy(o_rows(b, me), o_tok.at[b, :, mine(me, cols)], o_keep.at[even(b)])

    def keep_wo(h):
        return pltpu.make_async_copy(gw.src(h), wo_full.at[h, mine(me, cols), :], wo_keep.at[h])

    def remote(src, dst, send, recv, device):
        return pltpu.make_async_remote_copy(src_ref=src, dst_ref=dst, send_sem=send, recv_sem=recv, device_id=device, device_id_type=MESH)

    def share(n):
        buf, send, recv = sums[n]

        def work(b):
            for t in peers.at[1:]:
                remote(buf.at[me, b], buf.at[me, b], send, recv.at[b], {'tp': t}).start()
        return work

    def sum_of(n, b):
        return jnp.sum(sums[n][0][:, b], axis=0) * (1.0 / dim)

    def send_row(b):
        share(1)(b)
        for t in peers.at[1:]:
            remote(o_rows(b, t), o_tok.at[b, :, mine(me, cols)], o_send.at[even(b)], o_recv, {'tp': t}).start()
        keep_o(b).start()

    def wait_row_sent(b):
        wait_bytes(o_stage.at[even(b), pl.ds(0, seq - seg), :], o_send.at[even(b)])
        keep_o(b).wait()

    def pair_sends(b):
        for n in range(4):
            t = peers.at[1 ^ (2 * n)]
            remote(stage.at[mine(t, seg), :], pair_in.at[b, n], pair_send, pair_recv.at[b], {'tp': peers.at[1]}).start()

    def spread(row):
        return jnp.broadcast_to(row, (blk, blk)).T

    def turned(x, sl, kind):
        c, up, down = tabs[kind, sl, :], tabs[kind + 1, sl, :], tabs[kind + 2, sl, :]
        return x * c + pltpu.roll(x, HEAD_DIM - 1, 1) * up + pltpu.roll(x, 1, 1) * down

    def lane_cols(part, h):
        return pl.ds(part * cols + h * HEAD_DIM, HEAD_DIM)

    def load_y(b):
        gy.complete(b)

        @pl.when(b >= 1)
        def _():
            keep_y.wait()

        gy.load(b, y_slot, y_sem)

    def load_d(b):
        gd.complete(b)
        gd.load(b, d_slot.at[even(b)], d_sem.at[even(b)])

    def qkv(b):
        ring = lax.rem(b, 4)
        wait_local(y_slot, y_sem)
        pltpu.make_async_copy(y_slot.at[mine(me, seg), :], gy.piece(b, me), keep_sem).start()
        tile = 2 * blk
        for m in range(seq // tile):
            sl = pl.ds(m * tile, tile)
            acc = jnp.dot(y_slot[sl, :], w_all[...], preferred_element_type=F32) + bias[...]
            qk_ring[ring, sl, :] = acc[:, :wide]
            v_ring[even(b), sl, :] = acc[:, wide:].astype(BF16)
        for j in range(blocks):
            for part in range(2):
                total = None
                for h in range(heads):
                    x = qk_ring[ring, pl.ds(j * blk, blk), lane_cols(part, h)]
                    total = x * x if total is None else total + x * x
                norm_buf[me, b, pl.ds(part * blocks + j, 1), :] = jnp.sum(total.T, axis=0, keepdims=True)

    def inv_norms(b):
        return lax.rsqrt(sum_of(0, b) + EPS_NORM)

    def attend(b):
        s, ring = even(b), lax.rem(b, 4)
        wait_bytes(norm_buf.at[pl.ds(0, PARTS - 1), b], norm_recv.at[b])
        wait_local(d_slot.at[s], d_sem.at[s])

        @pl.when(b >= 2)
        def _():
            wait_row_sent(b - 2)
            out_copy(b - 2).wait()

        tile = 2 * blk
        for m in range(seq // tile):
            sl = pl.ds(m * tile, tile)
            datt[sl, :] = lax.dot_general(d_slot[s, sl, :], wo[...], COL_CONTRACT, preferred_element_type=F32).astype(BF16)

        inv = inv_norms(b)
        for j in range(blocks):
            sl = pl.ds(j * blk, blk)
            for part in range(2):
                row = part * blocks + j
                scale = spread(inv[row:row + 1, :])
                col_inv[s, part, sl, :] = scale
                for h in range(heads):
                    cs = lane_cols(part, h)
                    rot[sl, cs] = turned(qk_ring[ring, sl, cs] * scale * gains[:, cs], sl, 0).astype(BF16)

        def head(h, carry):
            hq, hk, hv = (pl.ds(pl.multiple_of(n * cols + h * HEAD_DIM, HEAD_DIM), HEAD_DIM) for n in range(3))
            k_h, v_h = rot[:, hk], v_ring[s, :, hq]
            for m in range(seq // tile):
                sl = pl.ds(m * tile, tile)
                sc = lax.dot_general(k_h, rot[sl, hq], COL_CONTRACT, preferred_element_type=F32) * SCORE_SCALE
                p = jnp.exp2(sc - jnp.max(sc, axis=0, keepdims=True))
                p = p * (1.0 / jnp.sum(p, axis=0, keepdims=True))
                dp = lax.dot_general(v_h, datt[sl, hq], COL_CONTRACT, preferred_element_type=F32)
                ds_buf[:, sl] = (p * (dp - jnp.sum(p * dp, axis=0, keepdims=True))).astype(BF16)
                p_buf[:, sl] = p.astype(BF16)
            dqk[:, hk] = jnp.dot(ds_buf[...], rot[:, hq], preferred_element_type=F32)
            dqkv_stage[s, :, hv] = jnp.dot(p_buf[...], datt[:, hq], preferred_element_type=F32).astype(BF16)
            o_stage[s, :, hq] = lax.dot_general(v_h, p_buf[...], ROW_CONTRACT, preferred_element_type=F32).T.astype(BF16)
            dqk[:, hq] = lax.dot_general(k_h, ds_buf[...], ROW_CONTRACT, preferred_element_type=F32).T
            return carry

        lax.fori_loop(0, heads, head, 0)

        for j in range(blocks):
            sl = pl.ds(j * blk, blk)
            for part in range(2):
                scale = col_inv[s, part, sl, :]
                total = None
                for h in range(heads):
                    cs = lane_cols(part, h)
                    dx = turned(dqk[sl, cs], sl, 3)
                    prod = dx * (qk_ring[ring, sl, cs] * scale)
                    dg_out[:, cs] = dg_out[:, cs] + jnp.sum(prod, axis=0, keepdims=True)
                    dqs[s, sl, cs] = dx * gains[:, cs]
                    prod = prod * gains[:, cs]
                    total = prod if total is None else total + prod
                stat_buf[me, b, pl.ds(part * blocks + j, 1), :] = jnp.sum(total.T, axis=0, keepdims=True)

        for n in range(3):
            cs = pl.ds(n * PANEL, PANEL)
            dwo_acc[:, cs] += lax.dot_general(o_stage[s], d_slot[s, :, cs], ROW_CONTRACT, preferred_element_type=F32)

    def finish(b):
        s, ring = even(b), lax.rem(b, 4)
        wait_bytes(stat_buf.at[pl.ds(0, PARTS - 1), b], stat_recv.at[b])
        inv = inv_norms(b)
        coef = sum_of(1, b) * inv * inv
        for j in range(blocks):
            sl = pl.ds(j * blk, blk)
            for part in range(2):
                row = part * blocks + j
                scale = col_inv[s, part, sl, :]
                pull = spread(coef[row:row + 1, :])
                for h in range(heads):
                    cs = lane_cols(part, h)
                    dqkv_stage[s, sl, cs] = (scale * dqs[s, sl, cs] - pull * qk_ring[ring, sl, cs]).astype(BF16)
        out_copy(b).start()
        for n in range(3):
            cs = pl.ds(n * PANEL, PANEL)
            stage[:, cs] = lax.dot_general(dqkv_stage[s], w_all[cs, :], COL_CONTRACT, preferred_element_type=F32).astype(BF16)

    def pair_sum(b):
        wait_bytes(pair_in.at[b], pair_recv.at[b])
        load = pltpu.make_async_copy(pair_in.at[b], pair_buf, pair_load)
        load.start()

        @pl.when(b >= 1)
        def _():
            pair_copy(b - 1).wait()

        wait_bytes(pair_in.at[b], pair_send)
        load.wait()
        for n in range(4):
            pair_stage[even(b), n] = (stage[mine(peers.at[2 * n], seg), :].astype(F32) + pair_buf[n].astype(F32)).astype(BF16)
        pair_copy(b).start()

    def spread_wo(h):
        gw.complete(h)
        for t in peers.at[1:]:
            piece = gw.piece(h, t)
            remote(piece, piece, z_send, z_recv, {'dp': 1 - depth}).start()

    def half_sends(b):
        for n, t in enumerate((peers.y, peers.x)):
            remote(pair_out.at[b, 3, mine(n, seg // 2), :], half_out.at[b, n], half_send.at[b], half_recv.at[n, b], {'tp': t}).start()

    def early_halves(lo, hi):
        def work(b):
            for n in range(lo, hi):
                half_sends(n)
        return work

    def step(i, carry):
        stage_of(i, 4, rows, send_row)
        stage_of(i, rows, 1, early_halves(0, 3))
        stage_of(i, rows + 1, 1, early_halves(6, 9))
        stage_of(i, rows + 2, 1, early_halves(9, 11))
        stage_of(i, rows + 3, 1, early_halves(11, 12))
        stage_of(i, rows + 4, 1, early_halves(12, 13))
        stage_of(i, rows + 5, 1, early_halves(13, EARLY))
        ahead_of(i, 2, rows, prepare(0))
        ahead_of(i, 1, rows, own_row(1))
        stage_of(i, 0, rows, gy.direct)
        stage_of(i, 1, rows, gy.diagonal)
        stage_of(i, 2, rows, load_d)
        stage_of(i, 2, 1, lambda b: gw.own(depth))
        stage_of(i, 4, 1, lambda b: gw.direct(depth))
        stage_of(i, 5, 1, lambda b: gw.diagonal(depth))
        stage_of(i, 6, 1, lambda b: spread_wo(depth))
        stage_of(i, 2, rows, qkv)
        stage_of(i, 6, rows, pair_sum)
        stage_of(i, 5, rows, finish)
        stage_of(i, 2, rows, share(0))
        stage_of(i, 5, rows, pair_sends)
        stage_of(i, rows, 1, early_halves(3, 6))
        ahead_of(i, 2, rows, prepare(1))
        ahead_of(i, 2, rows, own_row(0))
        stage_of(i, 0, rows, gd.direct)
        stage_of(i, 1, rows, gd.diagonal)
        stage_of(i, 1, rows, load_y)
        stage_of(i, 3, rows, attend)
        return carry

    keep_wo(0).start()
    keep_wo(1).start()
    lax.fori_loop(0, rows + 6, step, 0)
    stage[pl.ds(0, cols), :] = dwo_acc[...].astype(BF16)
    dwo_copy = pltpu.make_async_copy(stage.at[pl.ds(0, cols), :], dwo_out, dwo_sem)
    dwo_copy.start()
    keep_y.wait()
    keep_wo(0).wait()
    keep_wo(1).wait()
    for b in (rows - 2, rows - 1):
        wait_row_sent(b)
        out_copy(b).wait()
    pair_copy(rows - 1).wait()

    def drain(b, carry):
        gy.drain(b)
        gd.drain(b)
        return carry

    lax.fori_loop(0, rows, drain, 0)
    gw.drain(depth)
    for buf, send, _ in sums:
        wait_bytes(buf.at[pl.ds(0, PARTS - 1)], send)
    wait_bytes(o_tok.at[pl.ds(0, rows - rows // PARTS)], o_recv)
    sent = wo_full.at[0, pl.ds(0, dim - cols), :]
    wait_bytes(sent, z_send)
    wait_bytes(sent, z_recv)
    dwo_copy.wait()
    for b in range(EARLY):
        wait_bytes(half_out.at[b], half_send.at[b])
        for n in range(2):
            wait_bytes(half_out.at[b, n], half_recv.at[n, b])


def attend_grad(x_loc, d_out, w_q, w_k, w_v, small, w_o, mod_parts):
    rows, seg, dim = x_loc.shape
    cols = w_o.shape[0]
    seq = seg * PARTS
    hbm = pl.BlockSpec(memory_space=pl.ANY)
    vmem = pl.BlockSpec(memory_space=pltpu.VMEM)
    dma = pltpu.SemaphoreType.DMA
    two, each = dma((2,)), dma((rows,))
    gathered = jax.ShapeDtypeStruct((rows, seq, dim), BF16)
    paired = jax.ShapeDtypeStruct((rows, 4, seg, dim), BF16)
    local = jax.ShapeDtypeStruct((rows, seg, dim), BF16)
    local_ring = pltpu.VMEM((2, 2, seg, dim), BF16)
    wide, all_cols = 2 * cols, 3 * cols
    partials = pltpu.VMEM((PARTS, rows, 8, HEAD_DIM), F32)
    return pl.pallas_call(
        attend_kernel,
        out_shape=(local, local, gathered, gathered, jax.ShapeDtypeStruct((rows, seq, all_cols), BF16), jax.ShapeDtypeStruct((rows, seg, dim), BF16),
                   jax.ShapeDtypeStruct((2, dim, dim // 2), BF16), jax.ShapeDtypeStruct((cols, dim), BF16), paired, paired,
                   jax.ShapeDtypeStruct((EARLY, 2, seg // 2, dim), BF16),
                   jax.ShapeDtypeStruct((1, wide), F32)),
        in_specs=[hbm] * 5 + [vmem] * 10,
        out_specs=[hbm] * 11 + [vmem],
        scratch_shapes=[pltpu.VMEM((dim, all_cols), BF16), pltpu.VMEM((seq, dim), BF16), pltpu.VMEM((2, seq, dim), BF16),
                        pltpu.VMEM((4, seq, wide), F32), pltpu.VMEM((2, seq, cols), BF16), pltpu.VMEM((seq, wide), BF16),
                        pltpu.VMEM((2, seq, cols), BF16), pltpu.VMEM((seq, cols), BF16), pltpu.VMEM((seq, wide), F32),
                        pltpu.VMEM((2, seq, wide), F32), pltpu.VMEM((2, seq, all_cols), BF16), pltpu.VMEM((2, 2, seq, HEAD_DIM), F32),
                        pltpu.VMEM((seq, seq), BF16), pltpu.VMEM((seq, seq), BF16), pltpu.VMEM((cols, dim), F32), pltpu.VMEM((seq, dim), BF16),
                        pltpu.VMEM((2, 4, seg, dim), BF16), pltpu.VMEM((4, seg, dim), BF16),
                        partials, partials]
        + [[each] * 6, [each] * 6, [two] * 6, dma((3,)), dma, two, dma, dma, each, dma, each,
           two, two, dma, two, dma, each, dma, two, two, dma, dma, dma, dma((EARLY,)), dma((2, EARLY)),
           local_ring, local_ring, dma((2, 2)), dma((2, 2)),
           pltpu.VMEM((1, all_cols), F32), pltpu.VMEM((1, wide), F32), pltpu.VMEM((6, seq, HEAD_DIM), F32), pltpu.VMEM((3, rows, dim), F32)],
        compiler_params=pltpu.CompilerParams(collective_id=0, has_side_effects=True, vmem_limit_bytes=VMEM_ALL),
        name='gather_attend',
    )(x_loc, d_out, w_q, w_k, w_v, *small, w_o, *mod_parts)


def scatter_kernel(pairs, halves, dqkv, y_full, o_tok, wo_full, x_loc, d_out, e_rows, m_rows, b_o,
                   xo_out, dx_out, mod_out, dwq_out, dwk_out, dwv_out, half_in, last_in,
                   dt_slot, y_slot, half_stage, half_buf, last_buf, dw_acc,
                   o_all, x_all, dy_all, w_slot, proj, xo_stage, dx_stage, sums, mod_part, mod_in,
                   dt_sem, y_sem, half_send, last_send, half_recv0, half_recv1, last_recv0, last_recv1, half_load, last_load, dw_sem,
                   all_sem, wch_sem, xo_sem, dx_sem, part_send, part_recv, mod_send, mod_recv, mods):
    peers = Peers()
    me = peers.me
    rows, seq, dim = y_full.shape
    seg = seq // PARTS
    half = seg // 2
    cols = dim // PARTS
    width = w_slot.shape[2]
    chunks = dim // width
    group = mod_part.shape[2]
    every = [pltpu.make_async_copy(src, dst, all_sem.at[n]) for n, (src, dst) in enumerate(((o_tok, o_all), (x_loc, x_all), (d_out, dy_all)))]

    def mine(b, size):
        return pl.ds(pl.multiple_of(b * size, size), size)

    def dt_copy(b):
        return pltpu.make_async_copy(dqkv.at[b], dt_slot.at[even(b)], dt_sem.at[even(b)])

    def y_copy(b):
        return pltpu.make_async_copy(y_full.at[b], y_slot.at[even(b)], y_sem.at[even(b)])

    def dx_copy(b):
        return pltpu.make_async_copy(dx_stage.at[even(b)], dx_out.at[b], dx_sem.at[even(b)])

    def chunk_copy(n):
        per = chunks // 2
        return pltpu.make_async_copy(wo_full.at[n // per, :, mine(lax.rem(n, per), width)], w_slot.at[even(n)], wch_sem.at[even(n)])

    def xo_copy(n):
        return pltpu.make_async_copy(xo_stage.at[even(n)], xo_out.at[:, :, mine(n, width)], xo_sem.at[even(n)])

    def remote(src, dst, send, recv, t):
        pltpu.make_async_remote_copy(src_ref=src, dst_ref=dst, send_sem=send, recv_sem=recv,
                                     device_id={'tp': t}, device_id_type=MESH).start()

    def half_sends(b):
        remote(pairs.at[b, 3, pl.ds(0, half), :], half_in.at[b, 0], half_send.at[b], half_recv0.at[b], peers.y)
        remote(pairs.at[b, 3, pl.ds(half, half), :], half_in.at[b, 1], half_send.at[b], half_recv1.at[b], peers.x)

    ring = half_stage.shape[0]

    def last_sends(b):
        s = lax.rem(b, ring)
        remote(half_stage.at[s, 0], last_in.at[b, 0], last_send.at[b], last_recv0.at[b], peers.x)
        remote(half_stage.at[s, 1], last_in.at[b, 1], last_send.at[b], last_recv1.at[b], peers.y)

    def half_loads(b, source=None):
        s = even(b)
        return (pltpu.make_async_copy((half_in if source is None else source).at[b], half_buf.at[s], half_load.at[0, s]),
                pltpu.make_async_copy(pairs.at[b, pl.ds(1, 2)], half_stage.at[lax.rem(b, ring)], half_load.at[1, s]))

    def last_loads(b):
        return (pltpu.make_async_copy(last_in.at[b], last_buf.at[pl.ds(0, 2)], last_load.at[0]),
                pltpu.make_async_copy(pairs.at[b, 0], last_buf.at[2], last_load.at[1]))

    def fetch_half(b):
        @pl.when(b >= ring)
        def _():
            wait_bytes(last_in.at[b - ring], last_send.at[b - ring])

        @pl.when(b < EARLY)
        def _():
            for c in half_loads(b, halves):
                c.start()

        @pl.when(b >= EARLY)
        def _():
            wait_bytes(half_in.at[b, 0], half_recv0.at[b])
            wait_bytes(half_in.at[b, 1], half_recv1.at[b])
            for c in half_loads(b):
                c.start()

    def half_sum(b):
        s, r = even(b), lax.rem(b, ring)
        for c in half_loads(b):
            c.wait()
        for n in range(2):
            sl = pl.ds(n * half, half)
            half_stage[r, n, sl, :] = (half_stage[r, n, sl, :].astype(F32) + half_buf[s, n].astype(F32)).astype(BF16)

    def fetch_last(b):
        wait_bytes(last_in.at[b, 0], last_recv0.at[b])
        wait_bytes(last_in.at[b, 1], last_recv1.at[b])
        for c in last_loads(b):
            c.start()

    def last_sum(b):
        for c in last_loads(b):
            c.wait()

        @pl.when(b >= 2)
        def _():
            dx_copy(b - 2).wait()

        sums[...] = jnp.zeros_like(sums)
        few = FEW // 2
        scale = mods[1, pl.ds(b, 1), :]

        def tokens(n, carry):
            sl = mine(n, FEW)
            dy = last_buf[2, sl, :].astype(F32) + last_buf[0, sl, :].astype(F32) + last_buf[1, sl, :].astype(F32)
            x = x_all[b, sl, :].astype(F32)
            x = x - jnp.mean(x, axis=-1, keepdims=True)
            inv_std = lax.rsqrt(jnp.mean(x * x, axis=-1, keepdims=True) + EPS_NORM)
            x = x * inv_std
            sums[0] += dy[:few] + dy[few:]
            prod = dy * x
            sums[1] += prod[:few] + prod[few:]
            dn = dy * scale
            pull = x * jnp.mean(dn * x, axis=-1, keepdims=True) + jnp.mean(dn, axis=-1, keepdims=True)
            dx_stage[even(b), sl, :] = (dy_all[b, sl, :].astype(F32) + inv_std * (dn - pull)).astype(BF16)
            return carry

        lax.fori_loop(0, seg // FEW, tokens, 0)
        dx_copy(b).start()
        for n in range(2):
            mod_part[b // group, n, pl.ds(lax.rem(b, group), 1), :] = jnp.sum(sums[n], axis=0, keepdims=True)

    def project_out(n):
        cs = mine(n, width)

        @pl.when(n == 0)
        def _():
            for c in every:
                c.wait()

        @pl.when(n >= 2)
        def _():
            xo_copy(n - 2).wait()

        chunk_copy(n).wait()
        flat = o_all[...].reshape(rows * seg, dim)
        proj[...] = (jnp.dot(flat, w_slot[even(n)], preferred_element_type=F32) + b_o[:, cs]).reshape(proj.shape)

        def row(b, carry):
            out = proj[b]
            xo_stage[even(n), b] = (x_all[b, :, cs].astype(F32) + mods[2, pl.ds(b, 1), cs] * out).astype(BF16)
            mod_part[b // group, 2, pl.ds(lax.rem(b, group), 1), cs] = jnp.sum(dy_all[b, :, cs].astype(F32) * out, axis=0, keepdims=True)
            return carry

        lax.fori_loop(0, rows, row, 0)
        xo_copy(n).start()

        @pl.when(n + 2 < chunks)
        def _():
            chunk_copy(n + 2).start()

    def fetch_row(b):
        y_copy(b).start()
        dt_copy(b).start()

    def weight_grad(b):
        s = even(b)
        y_copy(b).wait()
        dt_copy(b).wait()
        for n in range(6):
            sl = pl.ds(n * (PANEL // 2), PANEL // 2)
            dw_acc[sl, :] += lax.dot_general(y_slot[s, :, sl], dt_slot[s], ROW_CONTRACT, preferred_element_type=F32)

    def share_parts(g):
        for t in peers.at[1:]:
            remote(mod_part.at[g, :, :, mine(t, cols)], mod_in.at[g, me], part_send.at[g], part_recv.at[g], t)
        mod_in[g, me] = mod_part[g, :, :, mine(me, cols)]

    def merge_parts(g):
        wait_bytes(mod_in.at[g, pl.ds(0, PARTS - 1)], part_recv.at[g])
        mod_out[g, :, :, mine(me, cols)] = jnp.sum(mod_in[g], axis=0)

    def share_mods(g):
        here = mod_out.at[g, :, :, mine(me, cols)]
        for t in peers.at[1:]:
            remote(here, here, mod_send.at[g], mod_recv.at[g], t)

    fetch_row(0)
    chunk_copy(0).start()
    chunk_copy(1).start()
    entry_barrier(peers, range(1, PARTS))
    for c in every:
        c.start()
    for b in range(EARLY, rows):
        half_sends(b)
    for b in range(2):
        fetch_half(b)
    fill_mods(mods, e_rows, m_rows)
    half_sum(0)
    half_sum(1)
    fetch_half(2)
    last_sends(0)
    dw_acc[...] = jnp.zeros_like(dw_acc)
    half_sum(2)
    last_sends(1)

    def step(i, carry):
        ahead_of(i, 2, rows, last_sends)
        ahead_of(i, 3, rows, fetch_half)
        stage_of(i, rows - 1, 1, share_parts)
        ahead_of(i, 1, rows, fetch_row)
        stage_of(i, 0, rows, weight_grad)
        stage_of(i, 2, rows, fetch_last)
        ahead_of(i, 3, rows, half_sum)
        stage_of(i, 1, chunks, project_out)
        stage_of(i, rows, 1, merge_parts)
        stage_of(i, rows + 1, 1, share_mods)
        stage_of(i, 2, rows, last_sum)
        return carry

    lax.fori_loop(0, rows + 2, step, 0)
    share_parts(1)
    tile = dt_slot.shape[1]
    turns = dim // tile
    own_cols = dwq_out.shape[1]
    copies = [[pltpu.make_async_copy(dt_slot.at[n % 2, :, pl.ds(k * own_cols, own_cols)], out.at[pl.ds(n * tile, tile), :], dw_sem.at[n, k])
               for k, out in enumerate((dwq_out, dwk_out, dwv_out))] for n in range(turns)]
    for n in range(turns):
        if n >= 2:
            for c in copies[n - 2]:
                c.wait()
        dt_slot[n % 2] = dw_acc[pl.ds(n * tile, tile), :].astype(BF16)
        for c in copies[n]:
            c.start()
    merge_parts(1)
    share_mods(1)
    for c in copies[turns - 2] + copies[turns - 1]:
        c.wait()
    for b in range(rows - ring, rows):
        wait_bytes(last_in.at[b], last_send.at[b])
    for n in range(2):
        dx_copy(rows - 1 - n).wait()
        xo_copy(chunks - 1 - n).wait()
    for b in range(EARLY, rows):
        wait_bytes(half_in.at[b], half_send.at[b])
    for g in range(2):
        some = mod_in.at[g, pl.ds(0, PARTS - 1)]
        wait_bytes(some, part_send.at[g])
        wait_bytes(some, mod_send.at[g])
        wait_bytes(some, mod_recv.at[g])


def scatter_grads(pairs, halves, dqkv, y_rows, o_rows, wo_full, x_loc, d_out, mod_parts, b_o):
    rows, seq, dim = y_rows.shape
    all_cols = dqkv.shape[2]
    seg = seq // PARTS
    group = rows // 2
    width = 256
    hbm = pl.BlockSpec(memory_space=pl.ANY)
    vmem = pl.BlockSpec(memory_space=pltpu.VMEM)
    dma = pltpu.SemaphoreType.DMA
    two, each = dma((2,)), dma((rows,))
    local = jax.ShapeDtypeStruct((rows, seg, dim), BF16)
    shard = pltpu.VMEM((rows, seg, dim), BF16)
    grad = jax.ShapeDtypeStruct((dim, all_cols // 3), BF16)
    return pl.pallas_call(
        scatter_kernel,
        out_shape=(local, local, jax.ShapeDtypeStruct((2, 3, group, dim), F32), grad, grad, grad,
                   jax.ShapeDtypeStruct((rows, 2, seg // 2, dim), BF16), jax.ShapeDtypeStruct((rows, 2, seg, dim), BF16)),
        in_specs=[hbm] * 8 + [vmem] * 3,
        out_specs=[hbm] * 2 + [vmem] + [hbm] * 5,
        scratch_shapes=[pltpu.VMEM((2, seq, all_cols), BF16), pltpu.VMEM((2, seq, dim), BF16),
                        pltpu.VMEM((8, 2, seg, dim), BF16), pltpu.VMEM((2, 2, seg // 2, dim), BF16),
                        pltpu.VMEM((3, seg, dim), BF16), pltpu.VMEM((dim, all_cols), F32),
                        shard, shard, shard, pltpu.VMEM((2, dim, width), BF16), pltpu.VMEM((rows, seg, width), F32),
                        pltpu.VMEM((2, rows, seg, width), BF16), pltpu.VMEM((2, seg, dim), BF16), pltpu.VMEM((2, FEW // 2, dim), F32),
                        pltpu.VMEM((2, 3, group, dim), F32), pltpu.VMEM((2, PARTS, 3, group, dim // PARTS), F32)]
        + [two, two] + [each] * 6 + [dma((2, 2)), two, dma((dim // seq, 3)), dma((3,))] + [two] * 7 + [pltpu.VMEM((3, rows, dim), F32)],
        compiler_params=pltpu.CompilerParams(collective_id=1, has_side_effects=True, vmem_limit_bytes=VMEM_ALL),
        name='grad_scatter',
    )(pairs, halves, dqkv, y_rows, o_rows, wo_full, x_loc, d_out, *mod_parts, b_o)


def solution(mesh):
    def device_step(x_loc, e_loc, m_block, w_q, b_q, w_k, b_k, w_v, b_v, w_o, b_o, g_q, g_k, pos_part, dy_loc):
        cols = w_q.shape[1]

        mod_parts = (jnp.moveaxis(e_loc, 1, 0), m_block)
        small = [b_q, b_k, b_v, g_q, g_k] + [jnp.repeat(t.T, 2, axis=0) for t in rope_angles(pos_part)]
        _, _, y_rows, _, dqkv, o_rows, wo_full, d_wo, _, pairs, halves, d_gains = attend_grad(x_loc, dy_loc, w_q, w_k, w_v, small, w_o, mod_parts)
        d_gq, d_gk = d_gains[0, :cols], d_gains[0, cols:]
        x_out, d_x, d_mods, d_wq, d_wk, d_wv = scatter_grads(pairs, halves, dqkv, y_rows, o_rows, wo_full, x_loc, dy_loc, mod_parts, b_o[None])[:6]
        d_mod = jnp.moveaxis(d_mods, 1, 2).reshape(e_loc.shape)
        return (x_out, d_x, d_mod, jnp.sum(d_mods, axis=(0, 2)), d_wq, d_wk, d_wv, d_wo, d_gq, d_gk)

    in_specs = (P('dp', 'tp', None), P('dp', None, None), P(None, None), P(None, 'tp'), P('tp'), P(None, 'tp'), P('tp'),
                P(None, 'tp'), P('tp'), P('tp', None), P(None), P('tp'), P('tp'), P('dp', None), P('dp', 'tp', None))
    out_specs = (P('dp', 'tp', None), P('dp', 'tp', None), P('dp', None, None), P('dp', None), P('dp', 'tp'), P('dp', 'tp'),
                 P('dp', 'tp'), P(('dp', 'tp'), None), P(('dp', 'tp')), P(('dp', 'tp')))
    return jax.shard_map(device_step, mesh=mesh, in_specs=in_specs, out_specs=out_specs, check_vma=False)
```

```python
import functools

import jax
import jax.numpy as jnp
from jax import lax
from jax.experimental import pallas as pl
from jax.experimental.pallas import tpu as pltpu
from jax.sharding import PartitionSpec as P

HEAD_DIM = 128
EPS_NORM = 1e-6
ROPE_BASE = 10000.0
ROW_CONTRACT = (((0,), (0,)), ((), ()))
COL_CONTRACT = (((1,), (1,)), ((), ()))
MESH = pl.DeviceIdType.MESH
F32 = jnp.float32
BF16 = jnp.bfloat16
PARTS = 8
PANEL = 1024
EARLY = 14
FEW = 16
VMEM_ALL = 67043328
SCORE_SCALE = HEAD_DIM ** -0.5 * 1.4426950408889634


def rope_angles(positions):
    half_dim = HEAD_DIM // 2
    side_len = HEAD_DIM // 6
    first_len = half_dim - 2 * side_len
    pair_idx = jnp.arange(half_dim)
    section = (pair_idx >= first_len).astype(jnp.int32) + (pair_idx >= first_len + side_len).astype(jnp.int32)
    offset = jnp.where(section == 0, 0, jnp.where(section == 1, first_len, first_len + side_len))
    sec_width = jnp.where(section == 0, first_len, side_len)
    freq_vals = ROPE_BASE ** (-(pair_idx - offset).astype(jnp.float32) / sec_width.astype(jnp.float32))
    select = jnp.where(section[None, :] == jnp.arange(3)[:, None], freq_vals[None, :], 0.0)
    angles = jnp.sum(positions.astype(jnp.float32)[:, :, None] * select[None, :, :], axis=1)
    return jnp.cos(angles), jnp.sin(angles)


def fill_tables(tabs, cos_tab, sin_tab):
    odd = lax.rem(lax.broadcasted_iota(jnp.int32, (1, HEAD_DIM), 1), 2).astype(F32)
    cos, sin = cos_tab[...].T, sin_tab[...].T
    up = sin * (odd - 1.0)
    down = sin * odd
    for n, (tab, scale) in enumerate(((cos, 1.0), (up, -1.0), (down, -1.0))):
        tabs[n] = tab
        tabs[n + 3] = tab * (scale * HEAD_DIM ** -0.5)


def fill_mods(mods, e_rows, m_rows):
    for n in range(3):
        mods[n] = e_rows[n] + m_rows[n:n + 1, :] + float(n == 1)


class Peers:
    def __init__(self):
        me = lax.axis_index('tp')
        self.me = me
        core, col, row = lax.rem(me, 2), lax.rem(me // 2, 2), me // 4

        def flip(bits):
            out = me
            if bits & 1:
                out = out + 1 - 2 * core
            if bits & 2:
                out = out + 2 - 4 * col
            if bits & 4:
                out = out + 4 - 8 * row
            return out

        self.at = [flip(bits) for bits in range(PARTS)]
        self.partner, self.x, self.y, self.diag = (self.at[bits] for bits in (1, 2, 4, 6))


def entry_barrier(peers, which):
    barrier = pltpu.get_barrier_semaphore()
    for bits in which:
        pl.semaphore_signal(barrier, inc=1, device_id={'tp': peers.at[bits]}, device_id_type=MESH)
    pl.semaphore_wait(barrier, len(which))


def wait_local(ref, sem):
    pltpu.make_async_copy(ref, ref, sem).wait()


def wait_bytes(ref, sem):
    pltpu.make_async_copy(ref, ref, sem).wait()


def even(b):
    return lax.rem(b, 2)


def third(b):
    return lax.rem(b, 3)


class RowGather:
    def __init__(self, peers, src, full, sems, seg):
        self.peers, self.src, self.full, self.seg = peers, src, full, seg
        self.send_sem, self.rx, self.ry, self.rd0, self.rd1, self.rp = sems
        self.lower, self.upper = (0, seg // 2), (seg // 2, seg // 2)

    def piece(self, b, t, part=None):
        lo, n = part or (0, self.seg)
        return self.full.at[b, pl.ds(pl.multiple_of(t * self.seg + lo, 32), n), :]

    def first(self, b, pieces):
        return self.full.at[b, pl.ds(0, pieces * self.seg), :]

    def send(self, src, dst, b, sem, t):
        pltpu.make_async_remote_copy(src_ref=src, dst_ref=dst, send_sem=self.send_sem.at[b], recv_sem=sem.at[b],
                                     device_id={'tp': t}, device_id_type=MESH).start()

    def own(self, b):
        p = self.peers
        for sem, t in ((self.rx, p.x), (self.ry, p.y), (self.rp, p.partner)):
            self.send(self.src(b), self.piece(b, p.me), b, sem, t)

    def direct(self, b):
        p = self.peers
        for near, sem, part, diag_sem, far in ((p.x, self.rx, self.lower, self.rd0, p.y), (p.y, self.ry, self.upper, self.rd1, p.x)):
            whole, some = self.piece(b, near), self.piece(b, near, part)
            wait_bytes(whole, sem.at[b])
            self.send(some, some, b, diag_sem, far)
            self.send(whole, whole, b, self.rp, p.partner)

    def diagonal(self, b):
        p = self.peers
        wait_bytes(self.piece(b, p.diag, self.lower), self.rd0.at[b])
        wait_bytes(self.piece(b, p.diag, self.upper), self.rd1.at[b])
        self.send(self.piece(b, p.diag), self.piece(b, p.diag), b, self.rp, p.partner)

    def complete(self, b):
        wait_bytes(self.first(b, 4), self.rp.at[b])

    def load(self, b, slot, sem):
        for n, t in enumerate(self.peers.at):
            src = self.piece(b, t) if n else self.src(b)
            pltpu.make_async_copy(src, slot.at[pl.ds(pl.multiple_of(t * self.seg, self.seg), self.seg), :], sem).start()

    def drain(self, b):
        wait_bytes(self.first(b, PARTS - 1), self.send_sem.at[b])


def stage_of(i, lag, count, work):
    @pl.when((i >= lag) & (i < count + lag))
    def _():
        work(i - lag)


def ahead_of(i, lead, count, work):
    stage_of(i + lead, lead, count - lead, lambda b: work(b + lead))


def attend_kernel(x_loc, d_out, wq, wk, wv, bq, bk, bv, gq, gk, cos_tab, sin_tab, wo, e_rows, m_rows,
                  y_own, d_own, y_full, dp_full, dqkv_out, o_tok, wo_full, dwo_out, pair_in, pair_out, half_out, dg_out,
                  w_all, y_slot, d_slot, qk_ring, v_ring, rot, o_stage, datt, dqk, dqs, dqkv_stage, col_inv, p_buf, ds_buf,
                  dwo_acc, stage, pair_stage, pair_buf, norm_buf, stat_buf,
                  y_sems, d_sems, wo_sems, w_sem, y_sem, d_sem, keep_sem, norm_send, norm_recv, stat_send, stat_recv,
                  o_send, o_keep, o_recv, out_sem, pair_send, pair_recv, pair_load, pair_sem, wo_keep, z_send, z_recv, dwo_sem, half_send, half_recv,
                  raw, own_stage, raw_sem, own_sem, bias, gains, tabs, mods):
    peers = Peers()
    me = peers.me
    depth = lax.axis_index('dp')
    sums = (norm_buf, norm_send, norm_recv), (stat_buf, stat_send, stat_recv)
    rows, seg, dim = x_loc.shape
    seq = seg * PARTS
    cols = wq.shape[1]
    heads = cols // HEAD_DIM
    blk = HEAD_DIM
    blocks = seq // blk
    wide = 2 * cols
    hemi = dim // 2
    weights = [pltpu.make_async_copy(w, w_all.at[:, pl.ds(n * cols, cols)], w_sem.at[n]) for n, w in enumerate((wq, wk, wv))]

    def raw_copy(kind, b):
        return pltpu.make_async_copy((x_loc, d_out)[kind].at[b], raw.at[kind, even(b)], raw_sem.at[kind, even(b)])

    def own_copy(kind, b):
        return pltpu.make_async_copy(own_stage.at[kind, even(b)], (y_own, d_own)[kind].at[b], own_sem.at[kind, even(b)])

    for b in range(2):
        raw_copy(0, b).start()
        raw_copy(1, b).start()
    for c in weights:
        c.start()
    fill_mods(mods, e_rows, m_rows)
    barrier = pltpu.get_barrier_semaphore()
    for t in peers.at[1:]:
        pl.semaphore_signal(barrier, inc=1, device_id={'tp': t}, device_id_type=MESH)
    pl.semaphore_signal(barrier, inc=1, device_id={'dp': 1 - depth}, device_id_type=MESH)
    pl.semaphore_wait(barrier, PARTS)
    gy = RowGather(peers, lambda b: y_own.at[b], y_full, y_sems, seg)
    gd = RowGather(peers, lambda b: d_own.at[b], dp_full, d_sems, seg)
    gw = RowGather(peers, lambda b: wo.at[:, pl.ds(pl.multiple_of(b * hemi, HEAD_DIM), hemi)], wo_full, wo_sems, cols)

    def prepare(kind):
        def work(b):
            raw_copy(kind, b).wait()
            s = even(b)
            shift, scale, gate = (mods[n, pl.ds(b, 1), :] for n in range(3))
            for n in range(seg // FEW):
                sl = pl.ds(n * FEW, FEW)
                x = raw[kind, s, sl, :].astype(F32)
                if kind == 0:
                    x = x - jnp.mean(x, axis=-1, keepdims=True)
                    x = x * lax.rsqrt(jnp.mean(x * x, axis=-1, keepdims=True) + EPS_NORM)
                    x = x * scale + shift
                else:
                    x = x * gate
                own_stage[kind, s, sl, :] = x.astype(BF16)
            own_copy(kind, b).start()

            @pl.when(b + 2 < rows)
            def _():
                raw_copy(kind, b + 2).start()
        return work

    def own_row(kind):
        def work(b):
            own_copy(kind, b).wait()
            (gy, gd)[kind].own(b)
        return work

    for kind, b in ((0, 0), (1, 0), (0, 1)):
        prepare(kind)(b)
        own_row(kind)(b)
    prepare(1)(1)
    fill_tables(tabs, cos_tab, sin_tab)
    for n, part in enumerate((bq, bk, bv)):
        bias[0, pl.ds(n * cols, cols)] = part[...]
    for n, part in enumerate((gq, gk)):
        gains[0, pl.ds(n * cols, cols)] = part[...]
    dwo_acc[...] = jnp.zeros_like(dwo_acc)
    dg_out[...] = jnp.zeros_like(dg_out)
    for c in weights:
        c.wait()

    def mine(b, width):
        return pl.ds(pl.multiple_of(b * width, width), width)

    keep_y = pltpu.make_async_copy(y_slot.at[mine(me, seg), :], gy.piece(0, me), keep_sem)

    def out_copy(b):
        return pltpu.make_async_copy(dqkv_stage.at[even(b)], dqkv_out.at[b], out_sem.at[even(b)])

    def pair_copy(b):
        return pltpu.make_async_copy(pair_stage.at[even(b)], pair_out.at[b], pair_sem.at[even(b)])

    def o_rows(b, t):
        return o_stage.at[third(b), mine(t, seg), :]

    def keep_o(b):
        return pltpu.make_async_copy(o_rows(b, me), o_tok.at[b, :, mine(me, cols)], o_keep.at[third(b)])

    def keep_wo(h):
        return pltpu.make_async_copy(gw.src(h), wo_full.at[h, mine(me, cols), :], wo_keep.at[h])

    def remote(src, dst, send, recv, device):
        return pltpu.make_async_remote_copy(src_ref=src, dst_ref=dst, send_sem=send, recv_sem=recv, device_id=device, device_id_type=MESH)

    def share(n):
        buf, send, recv = sums[n]

        def work(b):
            for t in peers.at[1:]:
                remote(buf.at[me, b], buf.at[me, b], send, recv.at[b], {'tp': t}).start()
        return work

    def sum_of(n, b):
        return jnp.sum(sums[n][0][:, b], axis=0) * (1.0 / dim)

    def send_row(b):
        for t in peers.at[1:]:
            remote(o_rows(b, t), o_tok.at[b, :, mine(me, cols)], o_send.at[third(b)], o_recv, {'tp': t}).start()
        keep_o(b).start()

    def wait_row_sent(b):
        wait_bytes(o_stage.at[third(b), pl.ds(0, seq - seg), :], o_send.at[third(b)])
        keep_o(b).wait()

    def pair_sends(b):
        for n in range(4):
            t = peers.at[1 ^ (2 * n)]
            remote(stage.at[mine(t, seg), :], pair_in.at[b, n], pair_send, pair_recv.at[b], {'tp': peers.at[1]}).start()

    def spread(row):
        return jnp.broadcast_to(row, (blk, blk)).T

    def turned(x, sl, kind):
        c, up, down = tabs[kind, sl, :], tabs[kind + 1, sl, :], tabs[kind + 2, sl, :]
        return x * c + pltpu.roll(x, HEAD_DIM - 1, 1) * up + pltpu.roll(x, 1, 1) * down

    def lane_cols(part, h):
        return pl.ds(part * cols + h * HEAD_DIM, HEAD_DIM)

    def load_y(b):
        gy.complete(b)

        @pl.when(b >= 1)
        def _():
            keep_y.wait()

        gy.load(b, y_slot, y_sem)

    def load_d(b):
        gd.complete(b)
        gd.load(b, d_slot.at[even(b)], d_sem.at[even(b)])

    def qkv(b):
        ring = lax.rem(b, 4)
        wait_local(y_slot, y_sem)
        pltpu.make_async_copy(y_slot.at[mine(me, seg), :], gy.piece(b, me), keep_sem).start()
        tile = 2 * blk
        for m in range(seq // tile):
            sl = pl.ds(m * tile, tile)
            acc = jnp.dot(y_slot[sl, :], w_all[...], preferred_element_type=F32) + bias[...]
            qk_ring[ring, sl, :] = acc[:, :wide]
            v_ring[even(b), sl, :] = acc[:, wide:].astype(BF16)
        for j in range(blocks):
            for part in range(2):
                total = None
                for h in range(heads):
                    x = qk_ring[ring, pl.ds(j * blk, blk), lane_cols(part, h)]
                    total = x * x if total is None else total + x * x
                norm_buf[me, b, pl.ds(part * blocks + j, 1), :] = jnp.sum(total.T, axis=0, keepdims=True)

    def inv_norms(b):
        return lax.rsqrt(sum_of(0, b) + EPS_NORM)

    def attend(b):
        s, ring = even(b), lax.rem(b, 4)
        wait_bytes(norm_buf.at[pl.ds(0, PARTS - 1), b], norm_recv.at[b])
        wait_local(d_slot.at[s], d_sem.at[s])

        @pl.when(b >= 3)
        def _():
            wait_row_sent(b - 3)

        @pl.when(b >= 2)
        def _():
            out_copy(b - 2).wait()

        tile = 2 * blk
        for m in range(seq // tile):
            sl = pl.ds(m * tile, tile)
            datt[sl, :] = lax.dot_general(d_slot[s, sl, :], wo[...], COL_CONTRACT, preferred_element_type=F32).astype(BF16)

        inv = inv_norms(b)
        for j in range(blocks):
            sl = pl.ds(j * blk, blk)
            for part in range(2):
                row = part * blocks + j
                scale = spread(inv[row:row + 1, :])
                col_inv[s, part, sl, :] = scale
                for h in range(heads):
                    cs = lane_cols(part, h)
                    rot[sl, cs] = turned(qk_ring[ring, sl, cs] * scale * gains[:, cs], sl, 0).astype(BF16)

        def head(h, carry):
            hq, hk, hv = (pl.ds(pl.multiple_of(n * cols + h * HEAD_DIM, HEAD_DIM), HEAD_DIM) for n in range(3))
            k_h, v_h = rot[:, hk], v_ring[s, :, hq]
            for m in range(seq // tile):
                sl = pl.ds(m * tile, tile)
                sc = lax.dot_general(k_h, rot[sl, hq], COL_CONTRACT, preferred_element_type=F32) * SCORE_SCALE
                p = jnp.exp2(sc - jnp.max(sc, axis=0, keepdims=True))
                p = p * (1.0 / jnp.sum(p, axis=0, keepdims=True))
                dp = lax.dot_general(v_h, datt[sl, hq], COL_CONTRACT, preferred_element_type=F32)
                ds_buf[:, sl] = (p * (dp - jnp.sum(p * dp, axis=0, keepdims=True))).astype(BF16)
                p_buf[:, sl] = p.astype(BF16)
            dqk[:, hk] = jnp.dot(ds_buf[...], rot[:, hq], preferred_element_type=F32)
            dqkv_stage[s, :, hv] = jnp.dot(p_buf[...], datt[:, hq], preferred_element_type=F32).astype(BF16)
            o_stage[third(b), :, hq] = lax.dot_general(v_h, p_buf[...], ROW_CONTRACT, preferred_element_type=F32).T.astype(BF16)
            dqk[:, hq] = lax.dot_general(k_h, ds_buf[...], ROW_CONTRACT, preferred_element_type=F32).T
            return carry

        lax.fori_loop(0, heads, head, 0)

        for j in range(blocks):
            sl = pl.ds(j * blk, blk)
            for part in range(2):
                scale = col_inv[s, part, sl, :]
                total = None
                for h in range(heads):
                    cs = lane_cols(part, h)
                    dx = turned(dqk[sl, cs], sl, 3)
                    prod = dx * (qk_ring[ring, sl, cs] * scale)
                    dg_out[:, cs] = dg_out[:, cs] + jnp.sum(prod, axis=0, keepdims=True)
                    dqs[s, sl, cs] = dx * gains[:, cs]
                    prod = prod * gains[:, cs]
                    total = prod if total is None else total + prod
                stat_buf[me, b, pl.ds(part * blocks + j, 1), :] = jnp.sum(total.T, axis=0, keepdims=True)

        for n in range(3):
            cs = pl.ds(n * PANEL, PANEL)
            dwo_acc[:, cs] += lax.dot_general(o_stage[third(b)], d_slot[s, :, cs], ROW_CONTRACT, preferred_element_type=F32)

    def finish(b):
        s, ring = even(b), lax.rem(b, 4)
        wait_bytes(stat_buf.at[pl.ds(0, PARTS - 1), b], stat_recv.at[b])
        inv = inv_norms(b)
        coef = sum_of(1, b) * inv * inv
        for j in range(blocks):
            sl = pl.ds(j * blk, blk)
            for part in range(2):
                row = part * blocks + j
                scale = col_inv[s, part, sl, :]
                pull = spread(coef[row:row + 1, :])
                for h in range(heads):
                    cs = lane_cols(part, h)
                    dqkv_stage[s, sl, cs] = (scale * dqs[s, sl, cs] - pull * qk_ring[ring, sl, cs]).astype(BF16)
        out_copy(b).start()
        for n in range(3):
            cs = pl.ds(n * PANEL, PANEL)
            stage[:, cs] = lax.dot_general(dqkv_stage[s], w_all[cs, :], COL_CONTRACT, preferred_element_type=F32).astype(BF16)

    def pair_sum(b):
        wait_bytes(pair_in.at[b], pair_recv.at[b])
        load = pltpu.make_async_copy(pair_in.at[b], pair_buf, pair_load)
        load.start()

        @pl.when(b >= 1)
        def _():
            pair_copy(b - 1).wait()

        wait_bytes(pair_in.at[b], pair_send)
        load.wait()
        for n in range(4):
            pair_stage[even(b), n] = (stage[mine(peers.at[2 * n], seg), :].astype(F32) + pair_buf[n].astype(F32)).astype(BF16)
        pair_copy(b).start()

    def spread_wo(h):
        gw.complete(h)
        for t in peers.at[1:]:
            piece = gw.piece(h, t)
            remote(piece, piece, z_send, z_recv, {'dp': 1 - depth}).start()

    def half_sends(b):
        for n, t in enumerate((peers.y, peers.x)):
            remote(pair_out.at[b, 3, mine(n, seg // 2), :], half_out.at[b, n], half_send.at[b], half_recv.at[n, b], {'tp': t}).start()

    def early_halves(lo, hi):
        def work(b):
            for n in range(lo, hi):
                half_sends(n)
        return work

    def step(i, carry):
        stage_of(i, rows, 1, early_halves(0, 3))
        stage_of(i, rows + 1, 1, early_halves(6, 9))
        stage_of(i, rows + 2, 1, early_halves(9, 11))
        stage_of(i, rows + 3, 1, early_halves(11, 12))
        stage_of(i, rows + 4, 1, early_halves(12, 13))
        stage_of(i, rows + 5, 1, early_halves(13, EARLY))
        stage_of(i, 0, rows, gy.direct)
        stage_of(i, 2, rows, gd.diagonal)
        stage_of(i, 6, rows, pair_sum)
        ahead_of(i, 2, rows, prepare(0))
        stage_of(i, 2, 1, lambda b: gw.own(depth))
        stage_of(i, 4, rows, share(1))
        ahead_of(i, 1, rows, own_row(1))
        stage_of(i, 4, 1, lambda b: gw.direct(depth))
        stage_of(i, 2, rows, qkv)
        stage_of(i, 5, 1, lambda b: gw.diagonal(depth))
        stage_of(i, 5, rows, send_row)
        stage_of(i, 6, 1, lambda b: spread_wo(depth))
        stage_of(i, 5, rows, finish)
        stage_of(i, rows, 1, early_halves(3, 6))
        ahead_of(i, 2, rows, prepare(1))
        stage_of(i, 5, rows, pair_sends)
        stage_of(i, 0, rows, gd.direct)
        stage_of(i, 2, rows, load_d)
        stage_of(i, 1, rows, load_y)
        stage_of(i, 2, rows, share(0))
        stage_of(i, 3, rows, attend)
        stage_of(i, 0, rows, gy.diagonal)
        ahead_of(i, 2, rows, own_row(0))
        return carry

    keep_wo(0).start()
    keep_wo(1).start()
    lax.fori_loop(0, rows + 6, step, 0)
    stage[pl.ds(0, cols), :] = dwo_acc[...].astype(BF16)
    dwo_copy = pltpu.make_async_copy(stage.at[pl.ds(0, cols), :], dwo_out, dwo_sem)
    dwo_copy.start()
    keep_y.wait()
    keep_wo(0).wait()
    keep_wo(1).wait()
    wait_row_sent(rows - 3)
    for b in (rows - 2, rows - 1):
        wait_row_sent(b)
        out_copy(b).wait()
    pair_copy(rows - 1).wait()

    def drain(b, carry):
        gy.drain(b)
        gd.drain(b)
        return carry

    lax.fori_loop(0, rows, drain, 0)
    gw.drain(depth)
    for buf, send, _ in sums:
        wait_bytes(buf.at[pl.ds(0, PARTS - 1)], send)
    wait_bytes(o_tok.at[pl.ds(0, rows - rows // PARTS)], o_recv)
    sent = wo_full.at[0, pl.ds(0, dim - cols), :]
    wait_bytes(sent, z_send)
    wait_bytes(sent, z_recv)
    dwo_copy.wait()
    for b in range(EARLY):
        wait_bytes(half_out.at[b], half_send.at[b])
        for n in range(2):
            wait_bytes(half_out.at[b, n], half_recv.at[n, b])


def attend_grad(x_loc, d_out, w_q, w_k, w_v, small, w_o, mod_parts):
    rows, seg, dim = x_loc.shape
    cols = w_o.shape[0]
    seq = seg * PARTS
    hbm = pl.BlockSpec(memory_space=pl.ANY)
    vmem = pl.BlockSpec(memory_space=pltpu.VMEM)
    dma = pltpu.SemaphoreType.DMA
    two, each = dma((2,)), dma((rows,))
    gathered = jax.ShapeDtypeStruct((rows, seq, dim), BF16)
    paired = jax.ShapeDtypeStruct((rows, 4, seg, dim), BF16)
    local = jax.ShapeDtypeStruct((rows, seg, dim), BF16)
    local_ring = pltpu.VMEM((2, 2, seg, dim), BF16)
    wide, all_cols = 2 * cols, 3 * cols
    partials = pltpu.VMEM((PARTS, rows, 8, HEAD_DIM), F32)
    return pl.pallas_call(
        attend_kernel,
        out_shape=(local, local, gathered, gathered, jax.ShapeDtypeStruct((rows, seq, all_cols), BF16), jax.ShapeDtypeStruct((rows, seg, dim), BF16),
                   jax.ShapeDtypeStruct((2, dim, dim // 2), BF16), jax.ShapeDtypeStruct((cols, dim), BF16), paired, paired,
                   jax.ShapeDtypeStruct((EARLY, 2, seg // 2, dim), BF16),
                   jax.ShapeDtypeStruct((1, wide), F32)),
        in_specs=[hbm] * 5 + [vmem] * 10,
        out_specs=[hbm] * 11 + [vmem],
        scratch_shapes=[pltpu.VMEM((dim, all_cols), BF16), pltpu.VMEM((seq, dim), BF16), pltpu.VMEM((2, seq, dim), BF16),
                        pltpu.VMEM((4, seq, wide), F32), pltpu.VMEM((2, seq, cols), BF16), pltpu.VMEM((seq, wide), BF16),
                        pltpu.VMEM((3, seq, cols), BF16), pltpu.VMEM((seq, cols), BF16), pltpu.VMEM((seq, wide), F32),
                        pltpu.VMEM((2, seq, wide), F32), pltpu.VMEM((2, seq, all_cols), BF16), pltpu.VMEM((2, 2, seq, HEAD_DIM), F32),
                        pltpu.VMEM((seq, seq), BF16), pltpu.VMEM((seq, seq), BF16), pltpu.VMEM((cols, dim), F32), pltpu.VMEM((seq, dim), BF16),
                        pltpu.VMEM((2, 4, seg, dim), BF16), pltpu.VMEM((4, seg, dim), BF16),
                        partials, partials]
        + [[each] * 6, [each] * 6, [two] * 6, dma((3,)), dma, two, dma, dma, each, dma, each,
           dma((3,)), dma((3,)), dma, two, dma, each, dma, two, two, dma, dma, dma, dma((EARLY,)), dma((2, EARLY)),
           local_ring, local_ring, dma((2, 2)), dma((2, 2)),
           pltpu.VMEM((1, all_cols), F32), pltpu.VMEM((1, wide), F32), pltpu.VMEM((6, seq, HEAD_DIM), F32), pltpu.VMEM((3, rows, dim), F32)],
        compiler_params=pltpu.CompilerParams(collective_id=0, has_side_effects=True, vmem_limit_bytes=VMEM_ALL),
        name='gather_attend',
    )(x_loc, d_out, w_q, w_k, w_v, *small, w_o, *mod_parts)


def scatter_kernel(pairs, halves, dqkv, y_full, o_tok, wo_full, x_loc, d_out, e_rows, m_rows, b_o,
                   xo_out, dx_out, mod_out, dwq_out, dwk_out, dwv_out, half_in, last_in,
                   dt_slot, y_slot, half_stage, half_buf, last_buf, dw_acc,
                   o_all, x_all, dy_all, w_slot, proj, xo_stage, dx_stage, sums, mod_part, mod_in,
                   dt_sem, y_sem, half_send, last_send, half_recv0, half_recv1, last_recv0, last_recv1, half_load, last_load, dw_sem,
                   all_sem, wch_sem, xo_sem, dx_sem, part_send, part_recv, mod_send, mod_recv, mods):
    peers = Peers()
    me = peers.me
    rows, seq, dim = y_full.shape
    seg = seq // PARTS
    half = seg // 2
    cols = dim // PARTS
    width = w_slot.shape[2]
    chunks = dim // width
    group = mod_part.shape[2]
    every = [pltpu.make_async_copy(src, dst, all_sem.at[n]) for n, (src, dst) in enumerate(((o_tok, o_all), (x_loc, x_all), (d_out, dy_all)))]

    def mine(b, size):
        return pl.ds(pl.multiple_of(b * size, size), size)

    def dt_copy(b):
        return pltpu.make_async_copy(dqkv.at[b], dt_slot.at[even(b)], dt_sem.at[even(b)])

    def y_copy(b):
        return pltpu.make_async_copy(y_full.at[b], y_slot.at[even(b)], y_sem.at[even(b)])

    def dx_copy(b):
        return pltpu.make_async_copy(dx_stage.at[even(b)], dx_out.at[b], dx_sem.at[even(b)])

    def chunk_copy(n):
        per = chunks // 2
        return pltpu.make_async_copy(wo_full.at[n // per, :, mine(lax.rem(n, per), width)], w_slot.at[even(n)], wch_sem.at[even(n)])

    def xo_copy(n):
        return pltpu.make_async_copy(xo_stage.at[even(n)], xo_out.at[:, :, mine(n, width)], xo_sem.at[even(n)])

    def remote(src, dst, send, recv, t):
        pltpu.make_async_remote_copy(src_ref=src, dst_ref=dst, send_sem=send, recv_sem=recv,
                                     device_id={'tp': t}, device_id_type=MESH).start()

    def half_sends(b):
        remote(pairs.at[b, 3, pl.ds(0, half), :], half_in.at[b, 0], half_send.at[b], half_recv0.at[b], peers.y)
        remote(pairs.at[b, 3, pl.ds(half, half), :], half_in.at[b, 1], half_send.at[b], half_recv1.at[b], peers.x)

    ring = half_stage.shape[0]

    def last_sends(b):
        s = lax.rem(b, ring)
        remote(half_stage.at[s, 0], last_in.at[b, 0], last_send.at[b], last_recv0.at[b], peers.x)
        remote(half_stage.at[s, 1], last_in.at[b, 1], last_send.at[b], last_recv1.at[b], peers.y)

    def half_loads(b, source=None):
        s = even(b)
        return (pltpu.make_async_copy((half_in if source is None else source).at[b], half_buf.at[s], half_load.at[0, s]),
                pltpu.make_async_copy(pairs.at[b, pl.ds(1, 2)], half_stage.at[lax.rem(b, ring)], half_load.at[1, s]))

    def last_loads(b):
        return (pltpu.make_async_copy(last_in.at[b], last_buf.at[pl.ds(0, 2)], last_load.at[0]),
                pltpu.make_async_copy(pairs.at[b, 0], last_buf.at[2], last_load.at[1]))

    def fetch_half(b):
        @pl.when(b >= ring)
        def _():
            wait_bytes(last_in.at[b - ring], last_send.at[b - ring])

        @pl.when(b < EARLY)
        def _():
            for c in half_loads(b, halves):
                c.start()

        @pl.when(b >= EARLY)
        def _():
            wait_bytes(half_in.at[b, 0], half_recv0.at[b])
            wait_bytes(half_in.at[b, 1], half_recv1.at[b])
            for c in half_loads(b):
                c.start()

    def half_sum(b):
        s, r = even(b), lax.rem(b, ring)
        for c in half_loads(b):
            c.wait()
        for n in range(2):
            sl = pl.ds(n * half, half)
            half_stage[r, n, sl, :] = (half_stage[r, n, sl, :].astype(F32) + half_buf[s, n].astype(F32)).astype(BF16)

    def fetch_last(b):
        wait_bytes(last_in.at[b, 0], last_recv0.at[b])
        wait_bytes(last_in.at[b, 1], last_recv1.at[b])
        for c in last_loads(b):
            c.start()

    def last_sum(b):
        for c in last_loads(b):
            c.wait()

        @pl.when(b >= 2)
        def _():
            dx_copy(b - 2).wait()

        sums[...] = jnp.zeros_like(sums)
        few = FEW // 2
        scale = mods[1, pl.ds(b, 1), :]

        def tokens(n, carry):
            sl = mine(n, FEW)
            dy = last_buf[2, sl, :].astype(F32) + last_buf[0, sl, :].astype(F32) + last_buf[1, sl, :].astype(F32)
            x = x_all[b, sl, :].astype(F32)
            x = x - jnp.mean(x, axis=-1, keepdims=True)
            inv_std = lax.rsqrt(jnp.mean(x * x, axis=-1, keepdims=True) + EPS_NORM)
            x = x * inv_std
            sums[0] += dy[:few] + dy[few:]
            prod = dy * x
            sums[1] += prod[:few] + prod[few:]
            dn = dy * scale
            pull = x * jnp.mean(dn * x, axis=-1, keepdims=True) + jnp.mean(dn, axis=-1, keepdims=True)
            dx_stage[even(b), sl, :] = (dy_all[b, sl, :].astype(F32) + inv_std * (dn - pull)).astype(BF16)
            return carry

        lax.fori_loop(0, seg // FEW, tokens, 0)
        dx_copy(b).start()
        for n in range(2):
            mod_part[b // group, n, pl.ds(lax.rem(b, group), 1), :] = jnp.sum(sums[n], axis=0, keepdims=True)

    def project_out(n):
        cs = mine(n, width)

        @pl.when(n == 0)
        def _():
            for c in every:
                c.wait()

        @pl.when(n >= 2)
        def _():
            xo_copy(n - 2).wait()

        chunk_copy(n).wait()
        flat = o_all[...].reshape(rows * seg, dim)
        proj[...] = (jnp.dot(flat, w_slot[even(n)], preferred_element_type=F32) + b_o[:, cs]).reshape(proj.shape)

        def row(b, carry):
            out = proj[b]
            xo_stage[even(n), b] = (x_all[b, :, cs].astype(F32) + mods[2, pl.ds(b, 1), cs] * out).astype(BF16)
            mod_part[b // group, 2, pl.ds(lax.rem(b, group), 1), cs] = jnp.sum(dy_all[b, :, cs].astype(F32) * out, axis=0, keepdims=True)
            return carry

        lax.fori_loop(0, rows, row, 0)
        xo_copy(n).start()

        @pl.when(n + 2 < chunks)
        def _():
            chunk_copy(n + 2).start()

    def fetch_row(b):
        y_copy(b).start()
        dt_copy(b).start()

    def weight_grad(b):
        s = even(b)
        y_copy(b).wait()
        dt_copy(b).wait()
        for n in range(6):
            sl = pl.ds(n * (PANEL // 2), PANEL // 2)
            dw_acc[sl, :] += lax.dot_general(y_slot[s, :, sl], dt_slot[s], ROW_CONTRACT, preferred_element_type=F32)

    def share_parts(g):
        for t in peers.at[1:]:
            remote(mod_part.at[g, :, :, mine(t, cols)], mod_in.at[g, me], part_send.at[g], part_recv.at[g], t)
        mod_in[g, me] = mod_part[g, :, :, mine(me, cols)]

    def merge_parts(g):
        wait_bytes(mod_in.at[g, pl.ds(0, PARTS - 1)], part_recv.at[g])
        mod_out[g, :, :, mine(me, cols)] = jnp.sum(mod_in[g], axis=0)

    def share_mods(g):
        here = mod_out.at[g, :, :, mine(me, cols)]
        for t in peers.at[1:]:
            remote(here, here, mod_send.at[g], mod_recv.at[g], t)

    fetch_row(0)
    chunk_copy(0).start()
    chunk_copy(1).start()
    entry_barrier(peers, range(1, PARTS))
    for c in every:
        c.start()
    for b in range(EARLY, rows):
        half_sends(b)
    for b in range(2):
        fetch_half(b)
    fill_mods(mods, e_rows, m_rows)
    half_sum(0)
    half_sum(1)
    fetch_half(2)
    last_sends(0)
    dw_acc[...] = jnp.zeros_like(dw_acc)
    half_sum(2)
    last_sends(1)

    def step(i, carry):
        ahead_of(i, 2, rows, last_sends)
        ahead_of(i, 3, rows, fetch_half)
        stage_of(i, rows - 1, 1, share_parts)
        ahead_of(i, 1, rows, fetch_row)
        stage_of(i, 0, rows, weight_grad)
        stage_of(i, 2, rows, fetch_last)
        ahead_of(i, 3, rows, half_sum)
        stage_of(i, 1, chunks, project_out)
        stage_of(i, rows, 1, merge_parts)
        stage_of(i, rows + 1, 1, share_mods)
        stage_of(i, 2, rows, last_sum)
        return carry

    lax.fori_loop(0, rows + 2, step, 0)
    share_parts(1)
    tile = dt_slot.shape[1]
    turns = dim // tile
    own_cols = dwq_out.shape[1]
    copies = [[pltpu.make_async_copy(dt_slot.at[n % 2, :, pl.ds(k * own_cols, own_cols)], out.at[pl.ds(n * tile, tile), :], dw_sem.at[n, k])
               for k, out in enumerate((dwq_out, dwk_out, dwv_out))] for n in range(turns)]
    for n in range(turns):
        if n >= 2:
            for c in copies[n - 2]:
                c.wait()
        dt_slot[n % 2] = dw_acc[pl.ds(n * tile, tile), :].astype(BF16)
        for c in copies[n]:
            c.start()
    merge_parts(1)
    share_mods(1)
    for c in copies[turns - 2] + copies[turns - 1]:
        c.wait()
    for b in range(rows - ring, rows):
        wait_bytes(last_in.at[b], last_send.at[b])
    for n in range(2):
        dx_copy(rows - 1 - n).wait()
        xo_copy(chunks - 1 - n).wait()
    for b in range(EARLY, rows):
        wait_bytes(half_in.at[b], half_send.at[b])
    for g in range(2):
        some = mod_in.at[g, pl.ds(0, PARTS - 1)]
        wait_bytes(some, part_send.at[g])
        wait_bytes(some, mod_send.at[g])
        wait_bytes(some, mod_recv.at[g])


def scatter_grads(pairs, halves, dqkv, y_rows, o_rows, wo_full, x_loc, d_out, mod_parts, b_o):
    rows, seq, dim = y_rows.shape
    all_cols = dqkv.shape[2]
    seg = seq // PARTS
    group = rows // 2
    width = 256
    hbm = pl.BlockSpec(memory_space=pl.ANY)
    vmem = pl.BlockSpec(memory_space=pltpu.VMEM)
    dma = pltpu.SemaphoreType.DMA
    two, each = dma((2,)), dma((rows,))
    local = jax.ShapeDtypeStruct((rows, seg, dim), BF16)
    shard = pltpu.VMEM((rows, seg, dim), BF16)
    grad = jax.ShapeDtypeStruct((dim, all_cols // 3), BF16)
    return pl.pallas_call(
        scatter_kernel,
        out_shape=(local, local, jax.ShapeDtypeStruct((2, 3, group, dim), F32), grad, grad, grad,
                   jax.ShapeDtypeStruct((rows, 2, seg // 2, dim), BF16), jax.ShapeDtypeStruct((rows, 2, seg, dim), BF16)),
        in_specs=[hbm] * 8 + [vmem] * 3,
        out_specs=[hbm] * 2 + [vmem] + [hbm] * 5,
        scratch_shapes=[pltpu.VMEM((2, seq, all_cols), BF16), pltpu.VMEM((2, seq, dim), BF16),
                        pltpu.VMEM((8, 2, seg, dim), BF16), pltpu.VMEM((2, 2, seg // 2, dim), BF16),
                        pltpu.VMEM((3, seg, dim), BF16), pltpu.VMEM((dim, all_cols), F32),
                        shard, shard, shard, pltpu.VMEM((2, dim, width), BF16), pltpu.VMEM((rows, seg, width), F32),
                        pltpu.VMEM((2, rows, seg, width), BF16), pltpu.VMEM((2, seg, dim), BF16), pltpu.VMEM((2, FEW // 2, dim), F32),
                        pltpu.VMEM((2, 3, group, dim), F32), pltpu.VMEM((2, PARTS, 3, group, dim // PARTS), F32)]
        + [two, two] + [each] * 6 + [dma((2, 2)), two, dma((dim // seq, 3)), dma((3,))] + [two] * 7 + [pltpu.VMEM((3, rows, dim), F32)],
        compiler_params=pltpu.CompilerParams(collective_id=1, has_side_effects=True, vmem_limit_bytes=VMEM_ALL),
        name='grad_scatter',
    )(pairs, halves, dqkv, y_rows, o_rows, wo_full, x_loc, d_out, *mod_parts, b_o)


def solution(mesh):
    def device_step(x_loc, e_loc, m_block, w_q, b_q, w_k, b_k, w_v, b_v, w_o, b_o, g_q, g_k, pos_part, dy_loc):
        cols = w_q.shape[1]

        mod_parts = (jnp.moveaxis(e_loc, 1, 0), m_block)
        small = [b_q, b_k, b_v, g_q, g_k] + [jnp.repeat(t.T, 2, axis=0) for t in rope_angles(pos_part)]
        _, _, y_rows, _, dqkv, o_rows, wo_full, d_wo, _, pairs, halves, d_gains = attend_grad(x_loc, dy_loc, w_q, w_k, w_v, small, w_o, mod_parts)
        d_gq, d_gk = d_gains[0, :cols], d_gains[0, cols:]
        x_out, d_x, d_mods, d_wq, d_wk, d_wv = scatter_grads(pairs, halves, dqkv, y_rows, o_rows, wo_full, x_loc, dy_loc, mod_parts, b_o[None])[:6]
        d_mod = jnp.moveaxis(d_mods, 1, 2).reshape(e_loc.shape)
        return (x_out, d_x, d_mod, jnp.sum(d_mods, axis=(0, 2)), d_wq, d_wk, d_wv, d_wo, d_gq, d_gk)

    in_specs = (P('dp', 'tp', None), P('dp', None, None), P(None, None), P(None, 'tp'), P('tp'), P(None, 'tp'), P('tp'),
                P(None, 'tp'), P('tp'), P('tp', None), P(None), P('tp'), P('tp'), P('dp', None), P('dp', 'tp', None))
    out_specs = (P('dp', 'tp', None), P('dp', 'tp', None), P('dp', None, None), P('dp', None), P('dp', 'tp'), P('dp', 'tp'),
                 P('dp', 'tp'), P(('dp', 'tp'), None), P(('dp', 'tp')), P(('dp', 'tp')))
    return jax.shard_map(device_step, mesh=mesh, in_specs=in_specs, out_specs=out_specs, check_vma=False)
```
